32 devices in a mesh: rep: 4 (over z), fsdp: 8 (over y, x, core).
Axes of the slice: x: 2, y: 2, z: 4, core: 2. Of those that a mesh axis runs over, the one named last changes fastest.
Arguments:
- x_tokens: bfloat16 [256, 257, 1024], P(('rep', 'fsdp'))
- grad_z: bfloat16 [256, 257, 1024], P(('rep', 'fsdp'))
- w_qkv: float32 [1024, 3072], P('fsdp')
- b_qkv: float32 [3072], P('fsdp')
- w_out: float32 [1024, 1024], P('fsdp')
- w_up: float32 [1024, 4096], P('fsdp')
- b_up: float32 [4096], P('fsdp')
- w_down: float32 [4096, 1024], P('fsdp')
- vec_params: float32 [8, 1024], P(None, 'fsdp')
Outputs:
- output 1: bfloat16 [256, 257, 1024], P(('rep', 'fsdp'))
- output 2: bfloat16 [256, 257, 1024], P(('rep', 'fsdp'))
- output 3: float32 [1024, 3072], P('fsdp')
- output 4: float32 [3072], P('fsdp')
- output 5: float32 [1024, 1024], P('fsdp')
- output 6: float32 [1024, 4096], P('fsdp')
- output 7: float32 [4096], P('fsdp')
- output 8: float32 [4096, 1024], P('fsdp')
- output 9: float32 [8, 1024], P(None, 'fsdp')
All inputs are finite; a program needn't handle non-finite values.
Results may differ from the reference program's by a relative error of at most 0.02.
Values are sent between devices in bfloat16 or wider.
A program may use at most 1 GiB of HBM per device.

```python
import jax
import jax.numpy as jnp
from jax import lax

D = 1024
FF = 4096
SEQ = 257
HEADS = 16
SEQS_DEV = 8
DEVICES = 32
BATCH = SEQS_DEV * DEVICES
HEAD = D // HEADS
LN_EPS = 1e-5


def setup_inputs(seed: int = 0) -> dict:
    keys = jax.random.split(jax.random.key(seed), 12)
    seq_scale = jax.random.uniform(keys[0], (BATCH, 1, 1), minval=0.5, maxval=2.0)
    x_tokens = (jax.random.normal(keys[1], (BATCH, SEQ, D)) * seq_scale).astype(jnp.bfloat16)
    grad_scale = jax.random.uniform(keys[2], (BATCH, 1, 1), minval=0.25, maxval=2.0)
    grad_z = (jax.random.normal(keys[3], (BATCH, SEQ, D)) * grad_scale).astype(jnp.bfloat16)
    w_qkv = jax.random.normal(keys[4], (D, 3 * D)) * D ** -0.5
    b_qkv = 0.5 * jax.random.normal(keys[5], (3 * D,))
    w_out = jax.random.normal(keys[6], (D, D)) * D ** -0.5
    w_up = jax.random.normal(keys[7], (D, FF)) * D ** -0.5
    b_up = 0.5 * jax.random.normal(keys[8], (FF,))
    w_down = jax.random.normal(keys[9], (FF, D)) * FF ** -0.5
    is_scale = jnp.array([0.0, 0.0, 0.0, 1.0, 0.0, 0.0, 0.0, 1.0], jnp.float32)[:, None]
    row_offset = jnp.array([1.0, 0.0, 0.0, 0.0, 1.0, 0.0, 0.0, 0.0], jnp.float32)[:, None]
    normal_rows = row_offset + 0.25 * jax.random.normal(keys[10], (8, D))
    scale_rows = jax.random.uniform(keys[11], (8, D), minval=0.5, maxval=1.5)
    vec_params = is_scale * scale_rows + (1.0 - is_scale) * normal_rows
    return {"x_tokens": x_tokens, "grad_z": grad_z, "w_qkv": w_qkv, "b_qkv": b_qkv, "w_out": w_out,
            "w_up": w_up, "b_up": b_up, "w_down": w_down, "vec_params": vec_params}


def normalize(t):
    mean = jnp.mean(t, axis=-1, keepdims=True)
    centered = t - mean
    variance = jnp.mean(centered * centered, axis=-1, keepdims=True)
    return centered * lax.rsqrt(variance + LN_EPS)


def gelu_exact(t):
    return jax.nn.gelu(t, approximate=False)


def layer_pass(x_seq, dz_seq, matrices, bias_qkv, bias_up, vec_rows):
    w_qkv, w_out, w_up, w_down = matrices
    ln1_gain, ln1_bias, out_bias, scale_attn, ln2_gain, ln2_bias, down_bias, scale_mlp = vec_rows
    score_scale = HEAD ** -0.5
    x_float = x_seq.astype(jnp.float32)
    xhat_one, norm_one_back = jax.vjp(normalize, x_float)
    h_one = (xhat_one * ln1_gain + ln1_bias).astype(jnp.bfloat16)
    qkv_proj = (jnp.dot(h_one, w_qkv, preferred_element_type=jnp.float32) + bias_qkv).astype(jnp.bfloat16)
    qkv_heads = qkv_proj.reshape(SEQ, 3, HEADS, HEAD).astype(jnp.float32)
    q_heads = qkv_heads[:, 0]
    k_heads = qkv_heads[:, 1]
    v_heads = qkv_heads[:, 2]
    scores = jnp.einsum("qhe,khe->hqk", q_heads, k_heads) * score_scale
    attn_probs = jax.nn.softmax(scores, axis=-1)
    probs_bf = attn_probs.astype(jnp.bfloat16).astype(jnp.float32)
    head_out = jnp.einsum("hqk,khe->qhe", probs_bf, v_heads).astype(jnp.bfloat16).reshape(SEQ, D)
    att_out = jnp.dot(head_out, w_out, preferred_element_type=jnp.float32) + out_bias
    resid_mid = x_float + scale_attn * att_out
    xhat_two, norm_two_back = jax.vjp(normalize, resid_mid)
    h_two = (xhat_two * ln2_gain + ln2_bias).astype(jnp.bfloat16)
    pre_act = jnp.dot(h_two, w_up, preferred_element_type=jnp.float32) + bias_up
    act_float, gelu_back = jax.vjp(gelu_exact, pre_act)
    mlp_act = act_float.astype(jnp.bfloat16)
    mlp_out = jnp.dot(mlp_act, w_down, preferred_element_type=jnp.float32) + down_bias
    z_seq = (resid_mid + scale_mlp * mlp_out).astype(jnp.bfloat16)
    g_out = dz_seq.astype(jnp.float32)
    grad_scale_mlp = jnp.sum(g_out * mlp_out, axis=0)
    d_mlp = g_out * scale_mlp
    grad_down_bias = jnp.sum(d_mlp, axis=0)
    d_mlp_bf = d_mlp.astype(jnp.bfloat16)
    grad_w_down = jnp.dot(mlp_act.T, d_mlp_bf, preferred_element_type=jnp.float32)
    d_act = jnp.dot(d_mlp_bf, w_down.T, preferred_element_type=jnp.float32)
    d_pre = gelu_back(d_act)[0]
    grad_b_up = jnp.sum(d_pre, axis=0)
    d_pre_bf = d_pre.astype(jnp.bfloat16)
    grad_w_up = jnp.dot(h_two.T, d_pre_bf, preferred_element_type=jnp.float32)
    d_h_two = jnp.dot(d_pre_bf, w_up.T, preferred_element_type=jnp.float32)
    grad_ln2_gain = jnp.sum(d_h_two * xhat_two, axis=0)
    grad_ln2_bias = jnp.sum(d_h_two, axis=0)
    g_resid = g_out + norm_two_back(d_h_two * ln2_gain)[0]
    grad_scale_attn = jnp.sum(g_resid * att_out, axis=0)
    d_att = g_resid * scale_attn
    grad_out_bias = jnp.sum(d_att, axis=0)
    d_att_bf = d_att.astype(jnp.bfloat16)
    grad_w_out = jnp.dot(head_out.T, d_att_bf, preferred_element_type=jnp.float32)
    d_heads = jnp.dot(d_att_bf, w_out.T, preferred_element_type=jnp.float32).astype(jnp.bfloat16)
    d_heads = d_heads.reshape(SEQ, HEADS, HEAD).astype(jnp.float32)
    d_probs = jnp.einsum("qhe,khe->hqk", d_heads, v_heads)
    grad_v = jnp.einsum("hqk,qhe->khe", probs_bf, d_heads)
    d_scores = attn_probs * (d_probs - jnp.sum(d_probs * attn_probs, axis=-1, keepdims=True))
    d_scores_bf = (d_scores * score_scale).astype(jnp.bfloat16).astype(jnp.float32)
    grad_q = jnp.einsum("hqk,khe->qhe", d_scores_bf, k_heads)
    grad_k = jnp.einsum("hqk,qhe->khe", d_scores_bf, q_heads)
    d_qkv = jnp.stack([grad_q, grad_k, grad_v], axis=1).reshape(SEQ, 3 * D)
    grad_b_qkv = jnp.sum(d_qkv, axis=0)
    d_qkv_bf = d_qkv.astype(jnp.bfloat16)
    grad_w_qkv = jnp.dot(h_one.T, d_qkv_bf, preferred_element_type=jnp.float32)
    d_h_one = jnp.dot(d_qkv_bf, w_qkv.T, preferred_element_type=jnp.float32)
    grad_ln1_gain = jnp.sum(d_h_one * xhat_one, axis=0)
    grad_ln1_bias = jnp.sum(d_h_one, axis=0)
    dx_seq = (g_resid + norm_one_back(d_h_one * ln1_gain)[0]).astype(jnp.bfloat16)
    grad_vec = jnp.stack([grad_ln1_gain, grad_ln1_bias, grad_out_bias, grad_scale_attn,
                          grad_ln2_gain, grad_ln2_bias, grad_down_bias, grad_scale_mlp])
    return z_seq, dx_seq, (grad_w_qkv, grad_b_qkv, grad_w_out, grad_w_up, grad_b_up, grad_w_down, grad_vec)


def reference(x_tokens, grad_z, w_qkv, b_qkv, w_out, w_up, b_up, w_down, vec_params):
    matrices = (w_qkv.astype(jnp.bfloat16), w_out.astype(jnp.bfloat16),
                w_up.astype(jnp.bfloat16), w_down.astype(jnp.bfloat16))
    bias_qkv = b_qkv.astype(jnp.bfloat16).astype(jnp.float32)
    bias_up = b_up.astype(jnp.bfloat16).astype(jnp.float32)
    vec_rows = vec_params.astype(jnp.bfloat16).astype(jnp.float32)

    def step(running, pair):
        z_seq, dx_seq, seq_grads = layer_pass(pair[0], pair[1], matrices, bias_qkv, bias_up, vec_rows)
        return jax.tree.map(jnp.add, running, seq_grads), (z_seq, dx_seq)

    zero_grads = (jnp.zeros((D, 3 * D), jnp.float32), jnp.zeros((3 * D,), jnp.float32),
                  jnp.zeros((D, D), jnp.float32), jnp.zeros((D, FF), jnp.float32),
                  jnp.zeros((FF,), jnp.float32), jnp.zeros((FF, D), jnp.float32),
                  jnp.zeros((8, D), jnp.float32))
    totals, seq_outs = lax.scan(step, zero_grads, (x_tokens, grad_z))
    grad_w_qkv, grad_b_qkv, grad_w_out, grad_w_up, grad_b_up, grad_w_down, grad_vec = totals
    return (seq_outs[0], seq_outs[1], grad_w_qkv, grad_b_qkv, grad_w_out, grad_w_up, grad_b_up,
            grad_w_down, grad_vec)
```

```python
import functools
import itertools

import jax
import jax.numpy as jnp
from jax import lax
from jax.experimental import pallas as pl
from jax.experimental.pallas import tpu as pltpu
from jax.sharding import PartitionSpec as P

F32 = jnp.float32
BF16 = jnp.bfloat16
LN_EPS = 1e-5
HEADS = 16
D = 1024
SEQ = 257
NSEQ = 8
PAD = 272
MAIN = 256
TAIL = PAD - MAIN
HEAD = D // HEADS
SCALE = HEAD ** -0.5
LOG2E = 1.4426950408889634
NEG = -1e30
QTR = 1024
ROWS = 128
LANES = 128
HD = D // 2
HH = HEADS // 2
PEERS = 8
DEPTH = 4
VMEM_MAX = 62 * 1024 * 1024
MESH = pl.DeviceIdType.MESH
ANY = pl.BlockSpec(memory_space=pl.ANY)
V_UP, V_QKV = 8, 12


def dot_nn(a, b):
    return lax.dot_general(a, b, (((1,), (0,)), ((), ())), preferred_element_type=F32)


def dot_nt(a, b):
    return lax.dot_general(a, b, (((1,), (1,)), ((), ())), preferred_element_type=F32)


def dot_tn(a, b):
    return lax.dot_general(a, b, (((0,), (0,)), ((), ())), preferred_element_type=F32)


def row_mean(t):
    return jnp.mean(t, axis=-1, keepdims=True)


def col_sum(t):
    return jnp.sum(t, axis=0, keepdims=True)


def ln_fwd(t):
    cen = t - row_mean(t)
    rstd = lax.rsqrt(row_mean(cen * cen) + LN_EPS)
    return cen * rstd, rstd


def ln_bwd(dxhat, xhat, rstd):
    return rstd * (dxhat - row_mean(dxhat) - xhat * row_mean(dxhat * xhat))


def sub8(t):
    return jnp.sum(t.reshape(t.shape[0] // 8, 8, t.shape[1]), axis=0)


def table_rows(ref, first=0, count=8):
    return [ref[k:k + 1] for k in range(first, first + count)]


def block(k):
    return slice(k * LANES, (k + 1) * LANES)


def params():
    return pltpu.CompilerParams(dimension_semantics=("arbitrary",), vmem_limit_bytes=VMEM_MAX)


def comm_params(cid):
    return pltpu.CompilerParams(dimension_semantics=("arbitrary",), vmem_limit_bytes=VMEM_MAX,
                                collective_id=cid, has_side_effects=True)


def fixed(shape):
    zeros = (0,) * len(shape)
    return pl.BlockSpec(shape, lambda *_: zeros, pipeline_mode=pl.Buffered(1))


def resident(shape):
    zeros = (0,) * len(shape)
    return pl.BlockSpec(shape, lambda *_: zeros)


def wblk(i):
    return pl.BlockSpec((PEERS, ROWS, D), lambda *_: (0, i, 0), pipeline_mode=pl.Buffered(1))


def one_seq(width=D, col=0):
    return pl.BlockSpec((None, PAD, width), lambda s: (s, 0, col))


def act(width=D, dtype=BF16):
    return jax.ShapeDtypeStruct((NSEQ, PAD, width), dtype)


def f32s(*shape):
    return jax.ShapeDtypeStruct(shape, F32)


def coords():
    me, z = lax.axis_index("fsdp"), lax.axis_index("rep")
    return z, me // 4, lax.rem(me // 2, 2), lax.rem(me, 2)


def index_of(name):
    _, y, x, c = coords()
    if "core" in name:
        c = 1 - c
    if "x" in name:
        x = 1 - x
    if "y" in name:
        y = 1 - y
    return 4 * y + 2 * x + c


def partner(name):
    z = lax.axis_index("rep")
    if name == "near":
        z = z + 1 - 2 * lax.rem(z, 2)
    elif name == "far":
        z = 3 - z
    return (z, index_of(name if name in ("core", "x", "y") else ""))


def is_inner():
    z = lax.axis_index("rep")
    return lax.rem(z + z // 2, 2)


def greet(devices, extra=0):
    sem = pltpu.get_barrier_semaphore()
    for dev in devices:
        pl.semaphore_signal(sem, inc=1, device_id=dev, device_id_type=MESH)
    pl.semaphore_wait(sem, len(devices) + extra)


def barrier(names):
    far = "far" in names
    inner = is_inner()
    if far:
        @pl.when(inner == 1)
        def _():
            pl.semaphore_signal(pltpu.get_barrier_semaphore(), inc=1, device_id=partner("far"), device_id_type=MESH)
    greet([partner(name) for name in names if name != "far"], inner if far else 0)


def remote(src, dst, sems, k, device):
    send_sem, recv_sem = sems
    return pltpu.make_async_remote_copy(src_ref=src, dst_ref=dst, send_sem=send_sem.at[k], recv_sem=recv_sem.at[k],
                                        device_id=device, device_id_type=MESH)


class Move:
    def __init__(self, copy, sender="every", receiver="every"):
        self.copy, self.sender, self.receiver = copy, sender, receiver

    def role(self, who, do):
        if who == "every":
            do()
        else:
            pl.when(is_inner() == int(who == "inner"))(do)

    def start(self):
        self.role(self.sender, self.copy.start)

    def recv(self):
        self.role(self.receiver, self.copy.wait_recv)

    def sent(self):
        self.role(self.sender, self.copy.wait_send)


ROLES = {"zA": ("outer", "inner"), "zB": ("inner", "inner"), "zC": ("inner", "outer")}
NAMES = {"s1": ("x", "y"), "s2": ("y", "x"), "zA": ("near",), "zB": ("far",), "zC": ("near",),
         "gather": ("core", "x", "y")}
GATHER_COPIES = 8
END = -1


def passes(shape):
    return shape[:1] + shape[2:] if len(shape) > 4 else shape


def kept_spec(shape):
    full = (shape[0], 1) + shape[2:] if len(shape) > 4 else shape
    zeros = (0,) * len(shape)
    return pl.BlockSpec(full, lambda *_: zeros, pipeline_mode=pl.Buffered(1))


class Chain:
    def __init__(self, array, first, *plan):
        plan = ((first, 0),) + plan
        self.array, self.stages, self.steps = array, [st for st, _ in plan], [step for _, step in plan]
        self.ends = self.stages[-1] == "zC"
        self.many = len(plan) > 1
        self.names = [nm for st in self.stages for nm in NAMES[st]]
        self.held = []
        shape = array.shape
        for _ in plan[1:]:
            shape = passes(shape)
            self.held.append(shape)
        self.kept, self.last = passes(shape), passes(shape)

    def args(self):
        return [self.array] * (1 + self.many)

    def in_specs(self):
        return [ANY, kept_spec(self.array.shape)][:1 + self.many]

    def results(self):
        kept = [(fixed(self.kept), self.kept)] * self.many
        return kept if self.many and self.ends else kept + [(ANY, self.last)]

    def scratch(self):
        return [pltpu.VMEM(shape, F32) for shape in self.held]

    def bind(self, ins, outs, held, sems, k):
        self.kept_out = outs[0]
        sources = ins[:1] + held
        targets = held + ([held[-1]] if self.many and self.ends else outs[-1:])
        if self.ends and not self.many:
            sources = outs[-1:]
        self.sums, self.adds, self.moves = held, ins[1:] + held, []
        for st, src, dst in zip(self.stages, sources, targets):
            moves = []
            for color, name in enumerate(NAMES[st]):
                a, b = (src.at[color, 1], dst.at[color]) if st in ("s1", "s2") else (src, dst)
                moves.append(Move(remote(a, b, sems, k, partner(name)), *ROLES.get(st, ())))
                k += 1
            self.moves.append(moves)
        return k

    def step(self, i):
        for n, (step, moves) in enumerate(zip(self.steps, self.moves)):
            @pl.when(i == step)
            def _(n=n, moves=moves):
                if n:
                    for mv in self.moves[n - 1]:
                        mv.recv()
                    held, kept = self.sums[n - 1], self.adds[n - 1]

                    def add():
                        mine = kept[:, 0] if len(kept.shape) > len(held.shape) else kept[:]
                        held[:] = held[:] + mine
                    if self.stages[n - 1] in ROLES:
                        pl.when(is_inner() == 1)(add)
                    else:
                        add()
                for mv in moves:
                    mv.start()

    def finish(self):
        for mv in self.moves[-1]:
            mv.recv()
        if self.many:
            held = self.sums[-1]
            self.kept_out[:] = held[:, 0] if len(held.shape) > len(self.kept) else held[:]
        for moves in self.moves:
            for mv in moves:
                mv.sent()


class Gather:
    names = NAMES["gather"]

    def __init__(self, buf, first, *steps):
        self.buf, self.plan = buf, [(first + j, step) for j, step in enumerate((0,) + steps)]

    def args(self):
        return [self.buf]

    def in_specs(self):
        return [ANY]

    def results(self):
        return [(ANY, self.buf.shape)]

    def scratch(self):
        return []

    def bind(self, ins, outs, held, sems, k):
        self.rounds = gather_moves(outs[0], sems, k)
        return k + GATHER_COPIES

    def step(self, i):
        for j, (rnd, step) in enumerate(self.plan):
            @pl.when(i == step)
            def _(j=j, rnd=rnd):
                if j:
                    pass_on([self.rounds], rnd)
                else:
                    for mv in self.rounds[rnd].every:
                        mv.start()

    def finish(self):
        for rnd, step in self.plan:
            if step == END:
                pass_on([self.rounds], rnd)
        for j, (rnd, _) in enumerate(self.plan):
            for mv in self.rounds[rnd].kept if j + 1 < len(self.plan) else self.rounds[rnd].every:
                mv.recv()
            for mv in self.rounds[rnd].every:
                mv.sent()


class Traffic:
    def __init__(self, items=(), extra=()):
        self.items = list(items)
        self.names = sorted({nm for item in self.items for nm in item.names} | set(extra))
        self.count = sum(GATHER_COPIES if isinstance(item, Gather) else len(item.names) for item in self.items)

    def arrays(self):
        return [arr for item in self.items for arr in item.args()]

    def in_specs(self):
        return [spec for item in self.items for spec in item.in_specs()]

    def out_specs(self):
        return [spec for item in self.items for spec, _ in item.results()]

    def out_shapes(self):
        return [jax.ShapeDtypeStruct(shape, item.args()[0].dtype) for item in self.items for _, shape in item.results()]

    def scratch(self):
        n = max(self.count, 1)
        held = [each for item in self.items for each in item.scratch()]
        return held + [pltpu.SemaphoreType.DMA((n,)), pltpu.SemaphoreType.DMA((n,))]

    def sizes(self):
        return len(self.in_specs()), len(self.out_specs()), len(self.scratch())

    def aliases(self, ins, outs):
        pairs = {}
        for item in self.items:
            if isinstance(item, Gather) or (item.ends and not item.many):
                pairs[ins] = outs
            ins, outs = ins + len(item.in_specs()), outs + len(item.results())
        return pairs

    def split(self, results):
        results, out = list(results), []
        for item in self.items:
            n = len(item.results())
            out.append(results[0] if n == 1 else tuple(results[:n]))
            results = results[n:]
        return out

    def begin(self, i, ins, outs, scratch):
        ins, outs, scratch = list(ins), list(outs), list(scratch)
        *scratch, send_sem, recv_sem = scratch
        k = 0
        for item in self.items:
            n, m, h = len(item.in_specs()), len(item.results()), len(item.scratch())
            k = item.bind(ins[:n], outs[:m], scratch[:h], (send_sem, recv_sem), k)
            ins, outs, scratch = ins[n:], outs[m:], scratch[h:]
        if self.names:
            @pl.when(i == 0)
            def _():
                barrier(self.names)
        for item in self.items:
            item.step(i)

    def finish(self, last):
        if self.items:
            @pl.when(last)
            def _():
                for item in self.items:
                    item.finish()


def pass_on(gathers, rnd):
    for rounds in gathers:
        for mv in rounds[rnd - 1].passed_on:
            mv.recv()
        for mv in rounds[rnd].every:
            mv.start()


class Round:
    def __init__(self, kept, passed_on):
        self.kept, self.passed_on, self.every = kept, passed_on, kept + passed_on


def gather_moves(buf, sems, k, own=None, rows=slice(None), half=None):
    n = buf.shape[1]
    me, at_x, at_y, at_xy = index_of(""), index_of("x"), index_of("y"), index_of("xy")
    low, high = half or (slice(0, n // 2), slice(n // 2, n))

    def mv(j, src, dst, name):
        return Move(remote(src, dst, sems, k + j, partner(name)))

    mine = buf.at[me, rows]
    first = [mv(j, mine if own is None else own, mine, name) for j, name in enumerate(NAMES["gather"])]
    second = [(at_x, rows, "core"), (at_y, rows, "core"), (at_y, low, "x"), (at_x, high, "y")]
    second = [mv(len(first) + j, buf.at[who, part], buf.at[who, part], name) for j, (who, part, name) in enumerate(second)]
    last = buf.at[at_xy, rows]
    third = [mv(len(first) + len(second), last, last, "core")]
    return Round(first[:1], first[1:]), Round(second[:2], second[2:]), Round(third, [])


def intake_kernel(xt, gt, wq, wo, wup, wdown, vecs, xp_ref, gp_ref, wall, wo_buf, *refs):
    (*ff_bufs, table_ref, xs, wide, wq_s, wo_s, up_s, down_s, own, ff_own, all_v,
     ssem, rsem, lsem) = refs
    me = index_of("")
    z = lax.axis_index("rep")
    loads = [pltpu.make_async_copy(src, dst, lsem.at[k]) for k, (src, dst) in enumerate((
        (wq, wq_s), (wo, wo_s), (wup, up_s), (wdown, down_s), (xt, xs.at[0]), (gt, xs.at[1])))]
    get_wq, get_wo, get_up, get_down, get_x, get_g = loads
    for cp in loads:
        cp.start()
    greet([(z, lax.rem(me + k, PEERS)) for k in range(1, PEERS)])
    vec_moves = [Move(remote(vecs, all_v.at[me], (ssem, rsem), k - 1, (z, lax.rem(me + k, PEERS))))
                 for k in range(1, PEERS)]
    for mv in vec_moves:
        mv.start()
    all_v[me] = vecs[:]
    get_wq.wait()
    stores, rounds = [], []

    def store(src, dst):
        cp = pltpu.make_async_copy(src, dst, lsem.at[len(loads) + len(stores)])
        cp.start()
        stores.append(cp)

    for t in range(3):
        part = slice(t * ROWS, (t + 1) * ROWS)
        own[part] = wq_s[:, t * D:(t + 1) * D].astype(BF16)
        mid = t * ROWS + ROWS // 2
        rounds.append(gather_moves(wall, (ssem, rsem), PEERS - 1 + t * GATHER_COPIES, own.at[part], part,
                                   (slice(t * ROWS, mid), slice(mid, (t + 1) * ROWS))))
        for mv in rounds[t][0].every:
            mv.start()
    store(own, wall.at[me])

    get_wo.wait()
    ff_own[DEPTH, :ROWS] = wo_s[:].astype(BF16)
    store(ff_own.at[DEPTH, pl.ds(0, ROWS)], wo_buf.at[me])
    get_up.wait()
    get_down.wait()
    for j, buf in enumerate(ff_bufs):
        for k in range(PEERS):
            ff_own[j, :ROWS, block(k)] = up_s[:, block(DEPTH * k + j)].astype(BF16)
        ff_own[j, ROWS:] = down_s[j * ROWS:(j + 1) * ROWS].astype(BF16)
        store(ff_own.at[j], buf.at[me])

    def by_sequence(t, out_ref):
        for k in range(PEERS):
            wide[k] = xs[t, :, :, block(k)].astype(F32).reshape(SEQ * NSEQ, LANES)
        out_ref[:, MAIN:PAD] = jnp.zeros((NSEQ, TAIL, D), BF16)

        @pl.loop(0, NSEQ)
        def _(s):
            for k in range(PEERS):
                out_ref[s, pl.ds(0, SEQ), block(k)] = wide[k, pl.ds(s, SEQ, stride=NSEQ), :].astype(BF16)

    get_x.wait()
    by_sequence(0, xp_ref)
    pass_on(rounds[:1], 1)
    get_g.wait()
    by_sequence(1, gp_ref)
    pass_on(rounds[1:], 1)
    for mv in vec_moves:
        mv.recv()
    for r in range(V_QKV):
        table_ref[r:r + 1] = jnp.concatenate([all_v[k, r:r + 1] for k in range(PEERS)], axis=1)
    flat = [all_v[k, V_QKV + t:V_QKV + t + 1] for k in range(PEERS) for t in range(3)]
    for t in range(3):
        table_ref[V_QKV + t:V_QKV + t + 1] = jnp.concatenate(flat[t * PEERS:(t + 1) * PEERS], axis=1)
    table_ref[:] = table_ref[:].astype(BF16).astype(F32)
    pass_on(rounds, 2)
    for first, second, third in rounds:
        for mv in first.kept + second.kept + third.every:
            mv.recv()
        for mv in first.every + second.every + third.every:
            mv.sent()
    for mv in vec_moves:
        mv.sent()
    for cp in stores:
        cp.wait()


def run_intake(xt, gt, wq, wo, wup, wdown, vecs, cid):
    copies = PEERS - 1 + 3 * GATHER_COPIES
    bufs = [jax.ShapeDtypeStruct((PEERS, n * ROWS, D), BF16) for n in (3, 1) + (2,) * DEPTH]
    vmem = pltpu.VMEM
    return pl.pallas_call(
        intake_kernel,
        in_specs=[ANY] * 6 + [pl.BlockSpec(memory_space=vmem)],
        out_specs=[pl.BlockSpec(memory_space=vmem)] * 2 + [ANY] * len(bufs) + [pl.BlockSpec(memory_space=vmem)],
        out_shape=[act(), act()] + bufs + [f32s(16, D)],
        scratch_shapes=[vmem((2, SEQ, NSEQ, D), BF16), vmem((PEERS, SEQ * NSEQ, LANES), F32),
                        vmem(wq.shape, F32), vmem(wo.shape, F32), vmem(wup.shape, F32), vmem(wdown.shape, F32),
                        vmem((3 * ROWS, D), BF16), vmem((DEPTH + 1, 2 * ROWS, D), BF16), vmem((PEERS, 16, LANES), F32),
                        pltpu.SemaphoreType.DMA((copies,)), pltpu.SemaphoreType.DMA((copies,)),
                        pltpu.SemaphoreType.DMA((6 + 2 + DEPTH,))],
        compiler_params=pltpu.CompilerParams(vmem_limit_bytes=VMEM_MAX, collective_id=cid, has_side_effects=True),
        name="intake",
    )(xt, gt, wq, wo, wup, wdown, vecs)


def qkv_kernel(traffic, x_ref, wq_ref, wk_ref, wv_ref, vec_ref, *refs):
    n_in, n_out, _ = traffic.sizes()
    srcs, (h_ref, q_ref, k_ref, v_ref, *refs) = refs[:n_in], refs[n_in:]
    i = pl.program_id(0)
    traffic.begin(i, srcs, refs[:n_out], refs[n_out:])
    rows = x_ref.shape[0] * PAD
    g1, c1, *_ = table_rows(vec_ref)
    xhat, _ = ln_fwd(x_ref[:].reshape(rows, D).astype(F32))
    h = (xhat * g1 + c1).astype(BF16)
    h_ref[:] = h.reshape(h_ref.shape)
    biases = table_rows(vec_ref, V_QKV, 3)
    for w_ref, o_ref, bias in zip((wq_ref, wk_ref, wv_ref), (q_ref, k_ref, v_ref), biases):
        o_ref[:] = (dot_nn(h, w_ref[:].reshape(D, D)) + bias).astype(BF16).reshape(o_ref.shape)
    traffic.finish(i == pl.num_programs(0) - 1)


def run_qkv(xp, wall, vec, cid, items):
    bs = 2
    traffic = Traffic(items)
    tok = pl.BlockSpec((bs, PAD, D), lambda s: (s, 0, 0))
    outs = pl.pallas_call(
        functools.partial(qkv_kernel, traffic), grid=(NSEQ // bs,),
        in_specs=[tok, wblk(0), wblk(1), wblk(2), fixed(vec.shape)] + traffic.in_specs(),
        out_specs=[tok] * 4 + traffic.out_specs(), out_shape=[act()] * 4 + traffic.out_shapes(),
        scratch_shapes=traffic.scratch(), input_output_aliases=traffic.aliases(5, 4),
        compiler_params=comm_params(cid), name="qkv",
    )(xp, wall, wall, wall, vec, *traffic.arrays())
    return outs[:4], traffic.split(outs[4:])


def low_lanes(rows):
    return lax.broadcasted_iota(jnp.int32, (rows, LANES), 1) < HEAD


def keys_mask(st):
    tail = st[MAIN:PAD]
    row = lax.broadcasted_iota(jnp.int32, tail.shape, 0)
    return jnp.concatenate([st[:MAIN], jnp.where(row < SEQ - MAIN, tail, NEG)], axis=0)


def diag_mask(heads):
    shape = (heads, heads * HEAD)
    row = lax.broadcasted_iota(jnp.int32, shape, 0)
    return lax.broadcasted_iota(jnp.int32, shape, 1) // HEAD == row


def last_by_head(t_ref, dmask, cols=slice(None)):
    last = t_ref[MAIN:PAD, cols][:1]
    return jnp.where(dmask, jnp.broadcast_to(last.astype(F32), dmask.shape), 0.0).astype(BF16)


def only_first_row(t):
    row = lax.broadcasted_iota(jnp.int32, (TAIL, t.shape[1]), 0)
    return jnp.where(row == 0, jnp.broadcast_to(t, row.shape), 0.0)


def softmax_t(st):
    st = keys_mask(st)
    m = jnp.max(st, axis=0, keepdims=True) * (SCALE * LOG2E)
    e = jnp.exp2(st * (SCALE * LOG2E) - m)
    total = col_sum(e)
    return e, total, m


def two_heads(t, low):
    zero = jnp.zeros(t.shape, t.dtype)
    return jnp.where(low, t, zero), jnp.where(low, zero, t)


def attn_fwd_kernel(traffic, q_ref, k_ref, v_ref, x_ref, g_ref, wo_ref, vec_ref, *refs):
    n_in, n_out, _ = traffic.sizes()
    srcs, (o_ref, a_ref, y_ref, h2_ref, dm_ref, lse_ref, *refs) = refs[:n_in], refs[n_in:]
    dsts, (s_s, p_s, *rest) = refs[:n_out], refs[n_out:]
    i = pl.program_id(0)
    traffic.begin(i, srcs, dsts, rest)
    low_q = low_lanes(MAIN)
    for p in range(HEADS // 2):
        halves = two_heads(q_ref[:MAIN, block(p)], low_q)
        for hh, qa in enumerate(halves):
            s_s[2 * p + hh] = dot_nt(k_ref[:, block(p)], qa)

    @pl.loop(0, 1)
    def _(t):
        for h in range(HEADS):
            e, total, m = softmax_t(s_s[h])
            p_s[h] = (e * (1.0 / total)).astype(BF16)
            lse_ref[h:h + 1, :] = m + jnp.log(total) * LOG2E

    for p in range(HEADS // 2):
        vt = v_ref[:, block(p)].T
        outs = [dot_nn(vt[hh * HEAD:(hh + 1) * HEAD], p_s[2 * p + hh]) for hh in range(2)]
        o_ref[:MAIN, block(p)] = jnp.concatenate(outs, axis=0).astype(BF16).T
    dmask = diag_mask(HEADS)
    e, total, _ = softmax_t(dot_nt(k_ref[:], last_by_head(q_ref, dmask)))
    ot = dot_tn((e * (1.0 / total)).astype(BF16), v_ref[:])
    o_ref[MAIN:PAD] = only_first_row(col_sum(jnp.where(dmask, ot, 0.0))).astype(BF16)

    _, _, bo, s1, g2, c2, _, s2 = table_rows(vec_ref)
    a = dot_nn(o_ref[:], wo_ref[:].reshape(D, D)) + bo
    a_ref[:] = a
    y = x_ref[:].astype(F32) + s1 * a
    y_ref[:] = y
    xhat, _ = ln_fwd(y)
    h2_ref[:] = (xhat * g2 + c2).astype(BF16)
    dm_ref[:] = (g_ref[:].astype(F32) * s2).astype(BF16)
    traffic.finish(i == NSEQ - 1)


def run_attn_fwd(q, k, v, xp, gp, wo, vec, cid, items):
    traffic = Traffic(items)
    tok = one_seq()
    outs = pl.pallas_call(
        functools.partial(attn_fwd_kernel, traffic), grid=(NSEQ,),
        in_specs=[tok] * 5 + [wblk(0), fixed(vec.shape)] + traffic.in_specs(),
        out_specs=[tok] * 5 + [pl.BlockSpec((None, HEADS, MAIN), lambda s: (s, 0, 0))] + traffic.out_specs(),
        out_shape=[act(), act(dtype=F32), act(dtype=F32), act(), act(), f32s(NSEQ, HEADS, MAIN)] + traffic.out_shapes(),
        scratch_shapes=[pltpu.VMEM((HEADS, PAD, MAIN), F32), pltpu.VMEM((HEADS, PAD, MAIN), BF16)] + traffic.scratch(),
        input_output_aliases=traffic.aliases(7, 6),
        compiler_params=comm_params(cid), name="attn_fwd",
    )(q, k, v, xp, gp, wo, vec, *traffic.arrays())
    return outs[:6], traffic.split(outs[6:])


def owner_rows(load, core):
    _, y, x, _ = coords()
    pieces = []
    for yy in (y, 1 - y):
        for xx in (x, 1 - x):
            pieces.append(load(pl.ds(pl.multiple_of((4 * yy + 2 * xx + core) * ROWS, ROWS), ROWS)))
    return jnp.concatenate(pieces, axis=1)


def store_piece(ab_ref, out, unit=0):
    w2 = out.shape[1] // 2
    for color in range(2):
        for ry in range(2):
            for rx in range(2):
                r = 2 * ry + rx
                sent, pos = (rx, ry) if color == 0 else (ry, rx)
                ab_ref[color, sent, pos, unit] = out[r * ROWS:(r + 1) * ROWS, color * w2:(color + 1) * w2]


class CorePair:
    def __init__(self, n, part_s, recv_s, sems, ab_ref):
        self.n, self.part_s, self.recv_s, self.ab_ref = n, part_s, recv_s, ab_ref
        self.copies = [Move(remote(part_s.at[k], recv_s.at[k], sems, k, partner("core"))) for k in range(n)]

    def step(self, k, product):
        core = lax.rem(lax.axis_index("fsdp"), 2)
        if 1 <= k <= self.n:
            self.copies[k - 1].start()
        if k < self.n:
            self.part_s[k] = product(k, 1 - core)
        else:
            unit = k - self.n
            out = product(unit, core)
            self.copies[unit].recv()
            self.copies[unit].sent()
            store_piece(self.ab_ref, out + self.recv_s[unit])


def pair_scratch(n, width):
    return [pltpu.VMEM((n, 4 * ROWS, width), F32), pltpu.VMEM((n, 4 * ROWS, width), F32),
            pltpu.SemaphoreType.DMA((n,)), pltpu.SemaphoreType.DMA((n,))]


def piece_spec(width, n, before):
    return pl.BlockSpec((2, 2, 2, 1, ROWS, width // 2),
                        lambda i: (0, 0, 0, jnp.clip(i - before, 0, n - 1), 0, 0))


def mlp_kernel(first, traffic, h2_ref, dm_ref, w1_ref, w2_ref, b1_ref, *refs):
    n_in, n_out, _ = traffic.sizes()
    if not first:
        m_in, dh_in, *refs = refs
    srcs, (m_out, dh_out, ab_ref, db_ref, *refs) = refs[:n_in], refs[n_in:]
    dsts, (act_s, du_s, part_s, recv_s, core_send, core_recv, *rest) = refs[:n_out], refs[n_out:]
    i = pl.program_id(0)
    bs = m_out.shape[0]
    rows = bs * PAD
    nblk = NSEQ // bs
    traffic.begin(i, srcs, dsts, rest)

    @pl.when(i == 0)
    def _():
        db_ref[:] = jnp.zeros_like(db_ref)

    @pl.when(i < nblk)
    def _():
        hb = h2_ref[pl.ds(i * bs, bs)].reshape(rows, D)
        dmb = dm_ref[pl.ds(i * bs, bs)].reshape(rows, D)
        w1 = w1_ref[:].reshape(D, QTR)
        w2 = w2_ref[:].reshape(QTR, D)
        mine = pl.ds(pl.multiple_of(i * rows, rows), rows)
        cw = 2 * LANES
        for c in range(QTR // cw):
            cols = slice(c * cw, (c + 1) * cw)
            u = dot_nn(hb, w1[:, cols]) + b1_ref[:, cols]
            da = dot_nt(dmb, w2[cols])
            cdf = 0.5 + 0.5 * lax.erf(u * (0.5 ** 0.5))
            slope = cdf + u * (jnp.exp(-0.5 * u * u) * 0.3989422804014327)
            du = da * slope
            db_ref[:, cols] += sub8(du)
            act_s[mine, cols] = (u * cdf).astype(BF16)
            du_s[mine, cols] = du.astype(BF16)
        m = dot_nn(act_s[mine, :], w2).reshape(m_out.shape)
        dh = dot_nt(du_s[mine, :], w1).reshape(dh_out.shape)
        m_out[:] = m if first else m_in[:] + m
        dh_out[:] = dh if first else dh_in[:] + dh

    flat = NSEQ * PAD
    pair = CorePair(2, part_s, recv_s, (core_send, core_recv), ab_ref)

    def product(which, core):
        if which == 0:
            return dot_tn(owner_rows(lambda lanes: h2_ref[:, :, lanes].reshape(flat, ROWS), core), du_s[:])
        return dot_tn(owner_rows(lambda lanes: act_s[:, lanes], core), dm_ref[:].reshape(flat, D))

    for k in range(4):
        @pl.when(i == nblk + k)
        def _(k=k):
            pair.step(k, product)

    traffic.finish(i == pl.num_programs(0) - 1)


def run_mlp(h2, dm, wff, b1, acc, cid, items=()):
    traffic = Traffic(items, ("core",))
    bs = 2
    nblk = NSEQ // bs
    tok = pl.BlockSpec((bs, PAD, D), lambda i: (jnp.minimum(i, nblk - 1), 0, 0))
    args = (h2, dm, wff, wff, b1) + acc
    base = len(args)
    outs = pl.pallas_call(
        functools.partial(mlp_kernel, not acc, traffic), grid=(nblk + 4,),
        in_specs=[fixed(h2.shape), fixed(dm.shape), wblk(0), wblk(1), fixed(b1.shape)] + [tok] * len(acc) + traffic.in_specs(),
        out_specs=[tok, tok, piece_spec(D, 2, nblk + 2), resident((8, QTR))] + traffic.out_specs(),
        out_shape=[act(dtype=F32), act(dtype=F32), f32s(2, 2, 2, 2, ROWS, HD), f32s(8, QTR)] + traffic.out_shapes(),
        scratch_shapes=[pltpu.VMEM((NSEQ * PAD, QTR), BF16), pltpu.VMEM((NSEQ * PAD, QTR), BF16)]
        + pair_scratch(2, D) + traffic.scratch(),
        input_output_aliases={**{base - len(acc) + k: k for k in range(len(acc))}, **traffic.aliases(base, 4)},
        compiler_params=comm_params(cid), name="mlp",
    )(*args, *traffic.arrays())
    m, dh, ab, db, *rest = outs
    return (m, dh), ab, db, traffic.split(rest)


ORDER = (("part", 0), ("part", 1), ("mine", 0), ("part", 2), ("mine", 1), ("part", 3), ("mine", 2), ("mine", 3))
EARLY = 2


def wgrad_kernel(traffic, h1, o, da, dq, dk, dv, *refs):
    n_in, n_out, _ = traffic.sizes()
    srcs, (ab_ref, *refs) = refs[:n_in], refs[n_in:]
    early, refs = refs[:EARLY], refs[EARLY:]
    dsts, (part_s, recv_s, core_send, core_recv, s1_send, s1_recv, *rest) = refs[:n_out], refs[n_out:]
    i = pl.program_id(0)
    flat = NSEQ * PAD
    core = lax.rem(lax.axis_index("fsdp"), 2)
    traffic.begin(i, srcs, dsts, rest)
    units = ((o, da), (h1, dv), (h1, dk), (h1, dq))
    across = [Move(remote(part_s.at[u % 2], recv_s.at[u], (core_send, core_recv), u, partner("core")))
              for u in range(len(units))]
    onward = [[Move(remote(ab_ref.at[color, 1, :, u], got.at[color], (s1_send, s1_recv), 2 * u + color, partner(nm)))
               for color, nm in enumerate(NAMES["s1"])] for u, got in enumerate(early)]

    def product(u, who):
        left, right = units[u]
        lhs = owner_rows(lambda lanes: left[:, :, lanes].reshape(flat, ROWS), who)
        return dot_tn(lhs, right[:].reshape(flat, D))

    for step, (what, u) in enumerate(ORDER):
        @pl.when(i == step)
        def _(step=step, what=what, u=u):
            before, prev = ORDER[step - 1]
            if step and before == "part":
                across[prev].start()
            if step and before == "mine" and prev < EARLY:
                for mv in onward[prev]:
                    mv.start()
            if what == "part":
                part_s[u % 2] = product(u, 1 - core)
            else:
                out = product(u, core)
                across[u].recv()
                across[u].sent()
                store_piece(ab_ref, out + recv_s[u], u)

    @pl.when(i == len(ORDER) - 1)
    def _():
        for moves in onward:
            for mv in moves:
                mv.recv()
                mv.sent()

    traffic.finish(i == len(ORDER) - 1)


def run_wgrad(ops, cid, items):
    traffic = Traffic(items, ("core", "x", "y"))
    n = DEPTH
    piece = (2, 2, 2, n, ROWS, HD)
    dma = pltpu.SemaphoreType.DMA
    outs = pl.pallas_call(
        functools.partial(wgrad_kernel, traffic), grid=(len(ORDER),),
        in_specs=[fixed(t.shape) for t in ops] + traffic.in_specs(),
        out_specs=[fixed(piece)] + [ANY] * EARLY + traffic.out_specs(),
        out_shape=[f32s(*piece)] + [f32s(2, 2, ROWS, HD)] * EARLY + traffic.out_shapes(),
        scratch_shapes=[pltpu.VMEM((2, 4 * ROWS, D), F32), pltpu.VMEM((n, 4 * ROWS, D), F32), dma((n,)), dma((n,)),
                        dma((2 * EARLY,)), dma((2 * EARLY,))] + traffic.scratch(),
        input_output_aliases=traffic.aliases(len(ops), 1 + EARLY),
        compiler_params=comm_params(cid), name="wgrad",
    )(*ops, *traffic.arrays())
    ab, *outs = outs
    return ab, outs[:EARLY], traffic.split(outs[EARLY:])


def heads_bwd(half, q_ref, k_ref, v_ref, do_ref, lse_ref, dq_ref, dk_ref, dv_ref, sum_ref,
              dk_s, dv_s, s_s, dp_s, p_s, ds_s):
    low_q, low_k = low_lanes(MAIN), low_lanes(PAD)
    pairs = HH // 2
    cols = slice(half * HD, (half + 1) * HD)
    for p in range(pairs):
        lanes = block(half * pairs + p)
        queries = two_heads(q_ref[:MAIN, lanes], low_q)
        cots = two_heads(do_ref[:MAIN, lanes], low_q)
        for hh in range(2):
            s_s[2 * p + hh] = dot_nt(k_ref[:, lanes], queries[hh])
            dp_s[2 * p + hh] = dot_nt(v_ref[:, lanes], cots[hh])

    @pl.loop(0, 1)
    def _(t):
        for h in range(HH):
            dpt = dp_s[h]
            lse = lse_ref[half * HH + h:half * HH + h + 1, :]
            prob = jnp.exp2(keys_mask(s_s[h]) * (SCALE * LOG2E) - lse)
            p_s[h] = prob.astype(BF16)
            ds_s[h] = (prob * (dpt - col_sum(prob * dpt)) * SCALE).astype(BF16)

    dmask = diag_mask(HH)
    qb, dob = last_by_head(q_ref, dmask, cols), last_by_head(do_ref, dmask, cols)
    e, total, _ = softmax_t(dot_nt(k_ref[:, cols], qb))
    prob = e * (1.0 / total)
    dp = dot_nt(v_ref[:, cols], dob)
    ds = (prob * (dp - col_sum(prob * dp)) * SCALE).astype(BF16)
    dv_s[:] = dot_nn(prob.astype(BF16), dob)
    dk_s[:] = dot_nn(ds, qb)
    dq_tail = only_first_row(col_sum(jnp.where(dmask, dot_tn(ds, k_ref[:, cols]), 0.0)))
    dq_ref[MAIN:PAD, cols] = dq_tail.astype(BF16)
    sum_ref[0, :, cols] += sub8(dq_tail)

    for p in range(pairs):
        lanes = block(half * pairs + p)
        q2, do2 = q_ref[:MAIN, lanes], do_ref[:MAIN, lanes]
        kt = k_ref[:, lanes].T
        heads = range(2 * p, 2 * p + 2)
        dv = jnp.where(low_k, *[dot_nn(p_s[h], do2) for h in heads]) + dv_s[:, block(p)]
        dk = jnp.where(low_k, *[dot_nn(ds_s[h], q2) for h in heads]) + dk_s[:, block(p)]
        dq = jnp.concatenate([dot_nn(kt[hh * HEAD:(hh + 1) * HEAD], ds_s[h]) for hh, h in enumerate(heads)], axis=0).T
        dv_ref[:, lanes] = dv.astype(BF16)
        dk_ref[:, lanes] = dk.astype(BF16)
        dq_ref[:MAIN, lanes] = dq.astype(BF16)
        for k, t in enumerate((dq, dk, dv)):
            sum_ref[k, :, lanes] += sub8(t)


def heads_scratch():
    scores = (HH, PAD, MAIN)
    return [pltpu.VMEM((PAD, HD), F32), pltpu.VMEM((PAD, HD), F32), pltpu.VMEM(scores, F32), pltpu.VMEM(scores, F32),
            pltpu.VMEM(scores, BF16), pltpu.VMEM(scores, BF16)]


def back_kernel(traffic, m_ref, y_ref, dh_ref, a_ref, g_ref, q_ref, k_ref, v_ref, lse_ref, wo_ref, vec_ref, *refs):
    n_in, n_out, _ = traffic.sizes()
    srcs, (z_ref, gres_ref, da_ref, dq_ref, dk_ref, dv_ref, sum_ref, hsum_ref, *refs) = refs[:n_in], refs[n_in:]
    dsts, (do_s, *refs) = refs[:n_out], refs[n_out:]
    n = len(heads_scratch())
    heads = refs[:n]
    i = pl.program_id(0)
    traffic.begin(i, srcs, dsts, refs[n:])

    @pl.when(i == 0)
    def _():
        sum_ref[:] = jnp.zeros_like(sum_ref)
        hsum_ref[:] = jnp.zeros_like(hsum_ref)

    _, _, _, s1, g2, _, b2, s2 = table_rows(vec_ref)
    g = g_ref[:].astype(F32)
    y = y_ref[:]
    m = m_ref[:] + b2
    z_ref[:] = (y + s2 * m).astype(BF16)[:SEQ]
    dh = dh_ref[:]
    xhat, rstd = ln_fwd(y)
    gres = g + ln_bwd(dh * g2, xhat, rstd)
    gres_ref[:] = gres
    da = gres * s1
    for k, t in enumerate((da, gres * a_ref[:], dh * xhat, dh, g * s2, g * m)):
        sum_ref[k] += sub8(t)
    dab = da.astype(BF16)
    da_ref[:] = dab
    do_s[:] = dot_nt(dab, wo_ref[:].reshape(D, D)).astype(BF16)
    for half in range(2):
        heads_bwd(half, q_ref, k_ref, v_ref, do_s, lse_ref, dq_ref, dk_ref, dv_ref, hsum_ref, *heads)
    traffic.finish(i == NSEQ - 1)


def run_back(m, y, dh, a, gp, q, k, v, lse, wo, vec, cid, items):
    traffic = Traffic(items)
    tok = one_seq()
    outs = pl.pallas_call(
        functools.partial(back_kernel, traffic), grid=(NSEQ,),
        in_specs=[tok] * 8 + [pl.BlockSpec((None, HEADS, MAIN), lambda s: (s, 0, 0)), wblk(0), fixed(vec.shape)]
        + traffic.in_specs(),
        out_specs=[pl.BlockSpec((None, SEQ, D), lambda s: (s, 0, 0))] + [tok] * 5
        + [resident((6, 8, D)), resident((3, 8, D))] + traffic.out_specs(),
        out_shape=[jax.ShapeDtypeStruct((NSEQ, SEQ, D), BF16), act(dtype=F32)] + [act()] * 4
        + [f32s(6, 8, D), f32s(3, 8, D)] + traffic.out_shapes(),
        scratch_shapes=[pltpu.VMEM((PAD, D), BF16)] + heads_scratch() + traffic.scratch(),
        input_output_aliases=traffic.aliases(11, 8),
        compiler_params=comm_params(cid), name="back",
    )(m, y, dh, a, gp, q, k, v, lse, wo, vec, *traffic.arrays())
    return outs[:8], traffic.split(outs[8:])


def adds_kernel(n, *refs):
    ins, outs = refs[:2 * n], refs[2 * n:]
    for a_ref, b_ref, o_ref in zip(ins[::2], ins[1::2], outs):
        o_ref[:] = a_ref[:].reshape(o_ref.shape) + b_ref[:].reshape(o_ref.shape)


def quarters(shape, kept=False):
    *lead, rows, width = shape
    lead = (1,) + ((1,) + tuple(lead[2:]) if kept else tuple(lead[1:]))
    zeros = (0,) * (len(lead) - 1)
    return pl.BlockSpec(lead + (rows // 2, width), lambda g: (g // 2,) + zeros + (lax.rem(g, 2), 0))


def run_adds(*jobs):
    specs, outs = [], []
    for a, b in jobs:
        outs.append(quarters(b.shape))
        specs += [quarters(a.shape, a.ndim > b.ndim), outs[-1]]
    return pl.pallas_call(
        functools.partial(adds_kernel, len(jobs)), grid=(4,), in_specs=specs, out_specs=outs,
        out_shape=[f32s(*b.shape) for _, b in jobs],
        compiler_params=params(), name="adds",
    )(*[t for job in jobs for t in job])


def store_ff(gup_ref, gdown_ref, f_ref, j):
    half = PEERS // 2
    for k in range(PEERS):
        gup_ref[:, block(DEPTH * k + j)] = f_ref[k // half, 0, :, block(k % half)]
    for color in range(2):
        gdown_ref[j * ROWS:(j + 1) * ROWS, color * HD:(color + 1) * HD] = f_ref[color, 1]


UNITS = DEPTH


def finish_kernel(x_ref, gres_ref, dq_ref, dk_ref, dv_ref, wq_ref, wk_ref, wv_ref, vec_ref, ab_any, keep_ref, e0, e1,
                  f0, f1, f2, p3_ref, b3_ref, sum_ref, hsum_ref, db0, db1, db2, db3,
                  dx_ref, gqkv_ref, gout_ref, gup_ref, gdown_ref, small_ref,
                  dx_s, ln_s, sk, r2, ra, rb, f3_s, small_s, all_p, part_s, all_z, ssem, rsem):
    i = pl.program_id(0)
    z, me = lax.axis_index("rep"), lax.axis_index("fsdp")
    sems, used = (ssem, rsem), []
    colors = range(2)

    def move(src, dst, device, *roles):
        used.append(Move(remote(src, dst, sems, len(used), device), *roles))
        return used[-1]

    s1 = {u: [move(ab_any.at[color, 1, :, u], sk.at[u, color], partner(nm)) for color, nm in enumerate(NAMES["s1"])]
          for u in range(EARLY, UNITS)}
    s2 = [[move(sk.at[u, color, 1], r2.at[u, color], partner(nm)) for color, nm in enumerate(NAMES["s2"])]
          for u in range(UNITS)]
    near, far = partner("near"), partner("far")
    z_a = [[move(sk.at[u, c, 0], ra.at[u, c], near, *ROLES["zA"]) for c in colors] for u in range(UNITS)]
    z_b = [[move(ra.at[u, c], rb.at[u, c], far, *ROLES["zB"]) for c in colors] for u in range(UNITS)]
    z_c = [[move(rb.at[u, c], rb.at[u, c], near, *ROLES["zC"]) for c in colors] for u in range(UNITS)]
    f3_c = move(f3_s, f3_s, near, *ROLES["zC"])
    others = [(z, lax.rem(me + k, PEERS)) for k in range(1, PEERS)]
    column = [(lax.rem(z + k, DEPTH), me) for k in range(1, DEPTH)]
    plane_moves = [move(small_s.at[to], all_p.at[me], (zz, to)) for zz, to in others]
    column_moves = [move(part_s, all_z.at[z], dev) for dev in column]

    def start(moves):
        for mv in moves:
            mv.start()

    def arrive(moves):
        for mv in moves:
            mv.recv()

    def inner(do):
        pl.when(is_inner() == 1)(do)

    def after_s1(u, came=None):
        if came is None:
            arrive(s1[u])
        for pos in (1, 0):
            for c in colors:
                got = sk[u, c, pos] if came is None else came[c, pos]
                sk[u, c, pos] = got + keep_ref[c, 0, pos, u]
        start(s2[u])

    def after_s2(u):
        arrive(s2[u])
        for c in colors:
            sk[u, c, 0] = sk[u, c, 0] + r2[u, c]
        start(z_a[u])

    def after_za(u):
        for c in colors:
            arrive(z_a[u][c:c + 1])

            @inner
            def _(c=c):
                ra[u, c] = ra[u, c] + sk[u, c, 0]
            start(z_b[u][c:c + 1])

    def after_zb(u):
        for c in colors:
            arrive(z_b[u][c:c + 1])

            @inner
            def _(c=c):
                rb[u, c] = rb[u, c] + ra[u, c]
            start(z_c[u][c:c + 1])

    @pl.when(i == 0)
    def _():
        greet(others + column)
        ln_s[:] = jnp.zeros_like(ln_s)

        @inner
        def _():
            f3_s[:] = p3_ref[:] + b3_ref[:]
        after_s1(0, e0)
        after_s1(1, e1)
        for u in s1:
            start(s1[u])
        start([f3_c])

    @pl.when(i == 4)
    def _():
        after_s2(0)
        after_s2(1)

    @pl.when(i == 7)
    def _():
        after_s1(2)
        after_za(0)

    dh = None
    for d_ref, w_ref in ((dq_ref, wq_ref), (dk_ref, wk_ref), (dv_ref, wv_ref)):
        part = dot_nt(d_ref[:], w_ref[:].reshape(D, D))
        dh = part if dh is None else dh + part
    g1, *_ = table_rows(vec_ref)
    xhat, rstd = ln_fwd(x_ref[:].astype(F32))
    for k, t in enumerate((dh * xhat, dh)):
        ln_s[k] += sub8(t)
    dx = gres_ref[:] + ln_bwd(dh * g1, xhat, rstd)
    for k in range(PEERS):
        dx_s[k, pl.ds(i, SEQ, stride=NSEQ), :] = dx[:SEQ, block(k)]

    @pl.when(i == NSEQ - 1)
    def _():
        rows = [col_sum(ref[k]) for ref in (ln_s, sum_ref) for k in range(ref.shape[0])]
        rows += [col_sum(ref[:]) for ref in (db0, db1, db2, db3)]
        blocks = [col_sum(hsum_ref[t])[:, block(k)] for t in range(3) for k in range(PEERS)]
        for to in range(PEERS):
            mine = [row[:, block(to)] for row in rows] + blocks[3 * to:3 * to + 3] + [jnp.zeros((1, LANES), F32)]
            small_s[to] = jnp.concatenate(mine, axis=0)
        start(plane_moves)
        all_p[me] = small_s[me]
        after_s1(3)
        after_za(1)
        after_zb(0)
        for k in range(PEERS):
            dx_ref[:, :, block(k)] = dx_s[k].reshape(SEQ, NSEQ, LANES).astype(BF16)
        arrive(plane_moves)
        part_s[:] = jnp.sum(all_p[:], axis=0)
        all_z[z] = part_s[:]
        start(column_moves)
        after_s2(2)
        for j, f_ref in enumerate((f0, f1, f2)):
            store_ff(gup_ref, gdown_ref, f_ref, j)
        after_zb(1)
        after_s2(3)
        after_za(2)
        arrive(column_moves)
        small_ref[:] = jnp.sum(all_z[:], axis=0)
        after_za(3)
        after_zb(2)
        after_zb(3)
        arrive([f3_c])
        store_ff(gup_ref, gdown_ref, f3_s, 3)
        for u, (out_ref, base) in enumerate(((gout_ref, 0), (gqkv_ref, 2 * D), (gqkv_ref, D), (gqkv_ref, 0))):
            for c in colors:
                arrive(z_c[u][c:c + 1])
                out_ref[:, base + c * HD:base + (c + 1) * HD] = rb[u, c]
        for mv in used:
            mv.sent()


def run_finish(xp, gres, grads, wall, vec, ab, early, ffs, last, sums, hsum, dbs, cid):
    tok = one_seq()
    outs = [(SEQ, NSEQ, D), (ROWS, 3 * D), (ROWS, D), (ROWS, DEPTH * D), (DEPTH * ROWS, D), (16, LANES)]

    def piece(*lead):
        return pltpu.VMEM(lead + (ROWS, HD), F32)

    scratch = [pltpu.VMEM((PEERS, SEQ * NSEQ, LANES), F32), pltpu.VMEM((2, 8, D), F32)]
    scratch += [piece(UNITS, 2, 2)] + [piece(UNITS, 2)] * 3 + [piece(2, 2)]
    scratch += [pltpu.VMEM((PEERS, 16, LANES), F32)] * 2
    scratch += [pltpu.VMEM((16, LANES), F32), pltpu.VMEM((DEPTH, 16, LANES), F32)]
    scratch += [pltpu.SemaphoreType.DMA((64,)), pltpu.SemaphoreType.DMA((64,))]
    consts = [sums, hsum] + list(dbs)
    held = [*early, *ffs, *last]
    before = [xp, gres, *grads, wall, wall, wall, vec, ab, ab, *held]
    return pl.pallas_call(
        finish_kernel, grid=(NSEQ,),
        in_specs=[tok] * 5 + [wblk(0), wblk(1), wblk(2), fixed(vec.shape), ANY, kept_spec(ab.shape)]
        + [fixed(t.shape) for t in held + consts],
        out_specs=[fixed(sh) for sh in outs],
        out_shape=[jax.ShapeDtypeStruct(outs[0], BF16)] + [f32s(*sh) for sh in outs[1:]],
        scratch_shapes=scratch, compiler_params=comm_params(cid), name="finish",
    )(*before, *consts)


def device_step(x_loc, dz_loc, w_qkv, b_qkv, w_out, w_up, b_up, w_down, vec_params):
    cid = itertools.count()
    vecs = jnp.concatenate([vec_params, b_up.reshape(-1, LANES), b_qkv.reshape(-1, LANES), jnp.zeros((1, LANES), F32)])
    xp, gp, wall, wo, c0, c1, c2, c3, vec = run_intake(
        x_loc.swapaxes(0, 1), dz_loc.swapaxes(0, 1), w_qkv, w_out, w_up, w_down, vecs, next(cid))
    b1 = [vec[V_UP + j:V_UP + j + 1] for j in range(DEPTH)]
    own, rest, last = range(3)
    (h1, q, k, v), (wo, c0) = run_qkv(xp, wall, vec, next(cid), [Gather(wo, own, 2, END), Gather(c0, own)])
    (o, a, y, h2, dm, lse), (c0, c1, c2) = run_attn_fwd(
        q, k, v, xp, gp, wo, vec, next(cid), [Gather(c0, rest, 3), Gather(c1, own), Gather(c2, own)])

    mlp = functools.partial(run_mlp, h2, dm)
    acc, f0, db0, (c1, c2, c3) = mlp(c0, b1[0], (), next(cid), [Gather(c1, rest, 3), Gather(c2, rest, 4), Gather(c3, own, 7)])
    acc, f1, db1, (c3, r0) = mlp(c1, b1[1], acc, next(cid), [Gather(c3, last), Chain(f0, "s1")])
    f0, = run_adds((f0, r0))
    acc, f2, db2, (r0, r1) = mlp(c2, b1[2], acc, next(cid), [Chain(f0, "s2", ("zA", 3)), Chain(f1, "s1")])
    f1, f0 = run_adds((f1, r1), r0)
    acc, f3, db3, (r1, r2, r0) = mlp(
        c3, b1[3], acc, next(cid), [Chain(f1, "s2", ("zA", 3)), Chain(f2, "s1"), Chain(f0, "zB")])
    f2, f1, f0 = run_adds((f2, r2), r1, (f0, r0))
    m, dh = acc
    (z, gres, da, dq, dk, dv, sums, hsum), (r2, r3, f1, f0) = run_back(
        m, y, dh, a, gp, q, k, v, lse, wo, vec, next(cid),
        [Chain(f2, "s2", ("zA", 2), ("zB", 5)), Chain(f3, "s1", ("s2", 5)), Chain(f1, "zB", ("zC", 4)), Chain(f0, "zC")])
    f3, f2 = run_adds(r3, r2)
    ab, early, (r3, f2) = run_wgrad([h1, o, da, dq, dk, dv], next(cid), [Chain(f3, "zA", ("zB", 6)), Chain(f2, "zC")])
    dx, g_qkv, g_out, g_up, g_down, small = run_finish(
        xp, gres, [dq, dk, dv], wall, vec, ab, early, [f0, f1, f2], r3, sums, hsum, [db0, db1, db2, db3], next(cid))
    g_bup, g_bqkv = small[V_UP:V_QKV].reshape(-1), small[V_QKV:V_QKV + 3].reshape(-1)
    return z, dx.swapaxes(0, 1), g_qkv, g_bqkv, g_out, g_up, g_bup, g_down, small[:V_UP]


def solution(mesh):
    batch = P(("rep", "fsdp"), None, None)
    row, flat, col = P("fsdp", None), P("fsdp"), P(None, "fsdp")
    par = (row, flat, row, row, flat, row, col)
    return jax.shard_map(device_step, mesh=mesh, in_specs=(batch, batch) + par,
                         out_specs=(batch, batch) + par, check_vma=False)
```

```python
import functools
import itertools

import jax
import jax.numpy as jnp
from jax import lax
from jax.experimental import pallas as pl
from jax.experimental.pallas import tpu as pltpu
from jax.sharding import PartitionSpec as P

F32 = jnp.float32
BF16 = jnp.bfloat16
LN_EPS = 1e-5
HEADS = 16
D = 1024
SEQ = 257
NSEQ = 8
PAD = 272
MAIN = 256
TAIL = PAD - MAIN
HEAD = D // HEADS
SCALE = HEAD ** -0.5
LOG2E = 1.4426950408889634
NEG = -1e30
QTR = 1024
ROWS = 128
LANES = 128
HD = D // 2
HH = HEADS // 2
PEERS = 8
DEPTH = 4
VMEM_MAX = 62 * 1024 * 1024
MESH = pl.DeviceIdType.MESH
ANY = pl.BlockSpec(memory_space=pl.ANY)
V_UP, V_QKV = 8, 12


def dot_nn(a, b):
    return lax.dot_general(a, b, (((1,), (0,)), ((), ())), preferred_element_type=F32)


def dot_nt(a, b):
    return lax.dot_general(a, b, (((1,), (1,)), ((), ())), preferred_element_type=F32)


def dot_tn(a, b):
    return lax.dot_general(a, b, (((0,), (0,)), ((), ())), preferred_element_type=F32)


def row_mean(t):
    return jnp.mean(t, axis=-1, keepdims=True)


def col_sum(t):
    return jnp.sum(t, axis=0, keepdims=True)


def ln_fwd(t):
    cen = t - row_mean(t)
    rstd = lax.rsqrt(row_mean(cen * cen) + LN_EPS)
    return cen * rstd, rstd


def ln_bwd(dxhat, xhat, rstd):
    return rstd * (dxhat - row_mean(dxhat) - xhat * row_mean(dxhat * xhat))


def sub8(t):
    return jnp.sum(t.reshape(t.shape[0] // 8, 8, t.shape[1]), axis=0)


def table_rows(ref, first=0, count=8):
    return [ref[k:k + 1] for k in range(first, first + count)]


def block(k):
    return slice(k * LANES, (k + 1) * LANES)


def params():
    return pltpu.CompilerParams(dimension_semantics=("arbitrary",), vmem_limit_bytes=VMEM_MAX)


def comm_params(cid):
    return pltpu.CompilerParams(dimension_semantics=("arbitrary",), vmem_limit_bytes=VMEM_MAX,
                                collective_id=cid, has_side_effects=True)


def fixed(shape):
    zeros = (0,) * len(shape)
    return pl.BlockSpec(shape, lambda *_: zeros, pipeline_mode=pl.Buffered(1))


def resident(shape):
    zeros = (0,) * len(shape)
    return pl.BlockSpec(shape, lambda *_: zeros)


def wblk(i):
    return pl.BlockSpec((PEERS, ROWS, D), lambda *_: (0, i, 0), pipeline_mode=pl.Buffered(1))


def one_seq(width=D, col=0):
    return pl.BlockSpec((None, PAD, width), lambda s: (s, 0, col))


def act(width=D, dtype=BF16):
    return jax.ShapeDtypeStruct((NSEQ, PAD, width), dtype)


def f32s(*shape):
    return jax.ShapeDtypeStruct(shape, F32)


def coords():
    me, z = lax.axis_index("fsdp"), lax.axis_index("rep")
    return z, me // 4, lax.rem(me // 2, 2), lax.rem(me, 2)


def index_of(name):
    _, y, x, c = coords()
    if "core" in name:
        c = 1 - c
    if "x" in name:
        x = 1 - x
    if "y" in name:
        y = 1 - y
    return 4 * y + 2 * x + c


def partner(name):
    z = lax.axis_index("rep")
    if name == "near":
        z = z + 1 - 2 * lax.rem(z, 2)
    elif name == "far":
        z = 3 - z
    return (z, index_of(name if name in ("core", "x", "y") else ""))


def is_inner():
    z = lax.axis_index("rep")
    return lax.rem(z + z // 2, 2)


def greet(devices, extra=0):
    sem = pltpu.get_barrier_semaphore()
    for dev in devices:
        pl.semaphore_signal(sem, inc=1, device_id=dev, device_id_type=MESH)
    pl.semaphore_wait(sem, len(devices) + extra)


def barrier(names):
    far = "far" in names
    inner = is_inner()
    if far:
        @pl.when(inner == 1)
        def _():
            pl.semaphore_signal(pltpu.get_barrier_semaphore(), inc=1, device_id=partner("far"), device_id_type=MESH)
    greet([partner(name) for name in names if name != "far"], inner if far else 0)


def remote(src, dst, sems, k, device):
    send_sem, recv_sem = sems
    return pltpu.make_async_remote_copy(src_ref=src, dst_ref=dst, send_sem=send_sem.at[k], recv_sem=recv_sem.at[k],
                                        device_id=device, device_id_type=MESH)


class Move:
    def __init__(self, copy, sender="every", receiver="every"):
        self.copy, self.sender, self.receiver = copy, sender, receiver

    def role(self, who, do):
        if who == "every":
            do()
        else:
            pl.when(is_inner() == int(who == "inner"))(do)

    def start(self):
        self.role(self.sender, self.copy.start)

    def recv(self):
        self.role(self.receiver, self.copy.wait_recv)

    def sent(self):
        self.role(self.sender, self.copy.wait_send)


ROLES = {"zA": ("outer", "inner"), "zB": ("inner", "inner"), "zC": ("inner", "outer")}
NAMES = {"s1": ("x", "y"), "s2": ("y", "x"), "zA": ("near", "near"), "zB": ("far", "far"), "zC": ("near", "near"),
         "gather": ("core", "x", "y")}
GATHER_COPIES = 8
END = -1
ONCE = 1


def passes(shape):
    return shape[:1] + shape[2:] if len(shape) > 4 else shape


def kept_spec(shape):
    full = (shape[0], 1) + shape[2:] if len(shape) > 4 else shape
    zeros = (0,) * len(shape)
    return pl.BlockSpec(full, lambda *_: zeros, pipeline_mode=pl.Buffered(1))


class Chain:
    def __init__(self, array, first, *plan):
        self.array = array
        self.stages = [first] + [st for st, *_ in plan]
        self.steps = [(0, 0)] + [(steps[0], steps[-1]) for _, *steps in plan]
        self.ends = self.stages[-1] == "zC"
        self.many = len(self.stages) > 1
        self.names = [nm for st in self.stages for nm in NAMES[st]]
        self.held = []
        shape = array.shape
        for _ in plan:
            shape = passes(shape)
            self.held.append(shape)
        self.kept, self.last = passes(shape), passes(shape)

    def args(self):
        return [self.array] * (1 + self.many)

    def in_specs(self):
        return [ANY, kept_spec(self.array.shape)][:1 + self.many]

    def results(self):
        kept = [(fixed(self.kept), self.kept)] * self.many
        return kept if self.many and self.ends else kept + [(ANY, self.last)]

    def scratch(self):
        return [pltpu.VMEM(shape, F32) for shape in self.held]

    def bind(self, ins, outs, held, sems, k):
        self.kept_out = outs[0]
        sources = ins[:1] + held
        targets = held + ([held[-1]] if self.many and self.ends else outs[-1:])
        if self.ends and not self.many:
            sources = outs[-1:]
        self.sums, self.adds, self.moves = held, ins[1:] + held, []
        for st, src, dst in zip(self.stages, sources, targets):
            moves = []
            for color, name in enumerate(NAMES[st]):
                a = src.at[color, 1] if st in ("s1", "s2") else src.at[color]
                moves.append(Move(remote(a, dst.at[color], sems, k, partner(name)), *ROLES.get(st, ())))
                k += 1
            self.moves.append(moves)
        return k

    def pass_on(self, n, color):
        if n:
            self.moves[n - 1][color].recv()
            held, kept = self.sums[n - 1], self.adds[n - 1]

            def add():
                mine = kept[color, 0] if len(kept.shape) > len(held.shape) else kept[color]
                held[color] = held[color] + mine
            if self.stages[n - 1] in ROLES:
                pl.when(is_inner() == 1)(add)
            else:
                add()
        self.moves[n][color].start()

    def step(self, i):
        for n, steps in enumerate(self.steps):
            for color, step in enumerate(steps):
                @pl.when(i == step)
                def _(n=n, color=color):
                    self.pass_on(n, color)

    def finish(self):
        for mv in self.moves[-1]:
            mv.recv()
        if self.many:
            held = self.sums[-1]
            self.kept_out[:] = held[:, 0] if len(held.shape) > len(self.kept) else held[:]
        for moves in self.moves:
            for mv in moves:
                mv.sent()


class Gather:
    names = NAMES["gather"]

    def __init__(self, buf, first, *steps, start=0):
        self.buf, self.plan = buf, [(first + j, step) for j, step in enumerate((start,) + steps)]

    def args(self):
        return [self.buf]

    def in_specs(self):
        return [ANY]

    def results(self):
        return [(ANY, self.buf.shape)]

    def scratch(self):
        return []

    def bind(self, ins, outs, held, sems, k):
        self.rounds = gather_moves(outs[0], sems, k)
        return k + GATHER_COPIES

    def step(self, i):
        for j, (rnd, step) in enumerate(self.plan):
            @pl.when(i == step)
            def _(j=j, rnd=rnd):
                if j:
                    pass_on([self.rounds], rnd)
                else:
                    for mv in self.rounds[rnd].every:
                        mv.start()

    def finish(self):
        for rnd, step in self.plan:
            if step == END:
                pass_on([self.rounds], rnd)
        for j, (rnd, _) in enumerate(self.plan):
            for mv in self.rounds[rnd].kept if j + 1 < len(self.plan) else self.rounds[rnd].every:
                mv.recv()
            for mv in self.rounds[rnd].every:
                mv.sent()


class Traffic:
    def __init__(self, items=(), extra=()):
        self.items = list(items)
        self.names = sorted({nm for item in self.items for nm in item.names} | set(extra))
        self.count = sum(GATHER_COPIES if isinstance(item, Gather) else len(item.names) for item in self.items)

    def arrays(self):
        return [arr for item in self.items for arr in item.args()]

    def in_specs(self):
        return [spec for item in self.items for spec in item.in_specs()]

    def out_specs(self):
        return [spec for item in self.items for spec, _ in item.results()]

    def out_shapes(self):
        return [jax.ShapeDtypeStruct(shape, item.args()[0].dtype) for item in self.items for _, shape in item.results()]

    def scratch(self):
        n = max(self.count, 1)
        held = [each for item in self.items for each in item.scratch()]
        return held + [pltpu.SemaphoreType.DMA((n,)), pltpu.SemaphoreType.DMA((n,))]

    def sizes(self):
        return len(self.in_specs()), len(self.out_specs()), len(self.scratch())

    def aliases(self, ins, outs):
        pairs = {}
        for item in self.items:
            if isinstance(item, Gather) or (item.ends and not item.many):
                pairs[ins] = outs
            ins, outs = ins + len(item.in_specs()), outs + len(item.results())
        return pairs

    def split(self, results):
        results, out = list(results), []
        for item in self.items:
            n = len(item.results())
            out.append(results[0] if n == 1 else tuple(results[:n]))
            results = results[n:]
        return out

    def begin(self, i, ins, outs, scratch):
        ins, outs, scratch = list(ins), list(outs), list(scratch)
        *scratch, send_sem, recv_sem = scratch
        k = 0
        for item in self.items:
            n, m, h = len(item.in_specs()), len(item.results()), len(item.scratch())
            k = item.bind(ins[:n], outs[:m], scratch[:h], (send_sem, recv_sem), k)
            ins, outs, scratch = ins[n:], outs[m:], scratch[h:]
        if self.names:
            @pl.when(i == 0)
            def _():
                barrier(self.names)
        for item in self.items:
            item.step(i)

    def finish(self, last):
        if self.items:
            @pl.when(last)
            def _():
                for item in self.items:
                    item.finish()


def pass_on(gathers, rnd):
    for rounds in gathers:
        for mv in rounds[rnd - 1].passed_on:
            mv.recv()
        for mv in rounds[rnd].every:
            mv.start()


class Round:
    def __init__(self, kept, passed_on):
        self.kept, self.passed_on, self.every = kept, passed_on, kept + passed_on


def gather_moves(buf, sems, k, own=None, rows=slice(None), half=None):
    n = buf.shape[1]
    me, at_x, at_y, at_xy = index_of(""), index_of("x"), index_of("y"), index_of("xy")
    low, high = half or (slice(0, n // 2), slice(n // 2, n))

    def mv(j, src, dst, name):
        return Move(remote(src, dst, sems, k + j, partner(name)))

    mine = buf.at[me, rows]
    first = [mv(j, mine if own is None else own, mine, name) for j, name in enumerate(NAMES["gather"])]
    second = [(at_x, rows, "core"), (at_y, rows, "core"), (at_y, low, "x"), (at_x, high, "y")]
    second = [mv(len(first) + j, buf.at[who, part], buf.at[who, part], name) for j, (who, part, name) in enumerate(second)]
    last = buf.at[at_xy, rows]
    third = [mv(len(first) + len(second), last, last, "core")]
    return Round(first[:1], first[1:]), Round(second[:2], second[2:]), Round(third, [])


def intake_kernel(xt, gt, wq, wo, wup, wdown, vecs, xp_ref, gp_ref, wall, wo_buf, *refs):
    (*ff_bufs, table_ref, xs, wide, wq_s, wo_s, up_s, down_s, own, ff_own, all_v,
     ssem, rsem, lsem) = refs
    me = index_of("")
    z = lax.axis_index("rep")
    loads = [pltpu.make_async_copy(src, dst, lsem.at[k]) for k, (src, dst) in enumerate((
        (wq, wq_s), (wo, wo_s), (wup, up_s), (wdown, down_s), (xt, xs.at[0]), (gt, xs.at[1])))]
    get_wq, get_wo, get_up, get_down, get_x, get_g = loads
    for cp in loads:
        cp.start()
    greet([(z, lax.rem(me + k, PEERS)) for k in range(1, PEERS)])
    vec_moves = [Move(remote(vecs, all_v.at[me], (ssem, rsem), k - 1, (z, lax.rem(me + k, PEERS))))
                 for k in range(1, PEERS)]
    for mv in vec_moves:
        mv.start()
    all_v[me] = vecs[:]
    get_wq.wait()
    stores, rounds = [], []

    def store(src, dst):
        cp = pltpu.make_async_copy(src, dst, lsem.at[len(loads) + len(stores)])
        cp.start()
        stores.append(cp)

    for t in range(3):
        part = slice(t * ROWS, (t + 1) * ROWS)
        own[part] = wq_s[:, t * D:(t + 1) * D].astype(BF16)
        mid = t * ROWS + ROWS // 2
        rounds.append(gather_moves(wall, (ssem, rsem), PEERS - 1 + t * GATHER_COPIES, own.at[part], part,
                                   (slice(t * ROWS, mid), slice(mid, (t + 1) * ROWS))))
        for mv in rounds[t][0].every:
            mv.start()
    store(own, wall.at[me])

    get_wo.wait()
    ff_own[DEPTH, :ROWS] = wo_s[:].astype(BF16)
    store(ff_own.at[DEPTH, pl.ds(0, ROWS)], wo_buf.at[me])
    get_up.wait()
    get_down.wait()
    for j, buf in enumerate(ff_bufs):
        for k in range(PEERS):
            ff_own[j, :ROWS, block(k)] = up_s[:, block(DEPTH * k + j)].astype(BF16)
        ff_own[j, ROWS:] = down_s[j * ROWS:(j + 1) * ROWS].astype(BF16)
        store(ff_own.at[j], buf.at[me])

    def by_sequence(t, out_ref):
        for k in range(PEERS):
            wide[k] = xs[t, :, :, block(k)].astype(F32).reshape(SEQ * NSEQ, LANES)
        out_ref[:, MAIN:PAD] = jnp.zeros((NSEQ, TAIL, D), BF16)

        @pl.loop(0, NSEQ)
        def _(s):
            for k in range(PEERS):
                out_ref[s, pl.ds(0, SEQ), block(k)] = wide[k, pl.ds(s, SEQ, stride=NSEQ), :].astype(BF16)

    get_x.wait()
    by_sequence(0, xp_ref)
    pass_on(rounds[:1], 1)
    get_g.wait()
    by_sequence(1, gp_ref)
    pass_on(rounds[1:], 1)
    for mv in vec_moves:
        mv.recv()
    for r in range(V_QKV):
        table_ref[r:r + 1] = jnp.concatenate([all_v[k, r:r + 1] for k in range(PEERS)], axis=1)
    flat = [all_v[k, V_QKV + t:V_QKV + t + 1] for k in range(PEERS) for t in range(3)]
    for t in range(3):
        table_ref[V_QKV + t:V_QKV + t + 1] = jnp.concatenate(flat[t * PEERS:(t + 1) * PEERS], axis=1)
    table_ref[:] = table_ref[:].astype(BF16).astype(F32)
    pass_on(rounds, 2)
    for first, second, third in rounds:
        for mv in first.kept + second.kept + third.every:
            mv.recv()
        for mv in first.every + second.every + third.every:
            mv.sent()
    for mv in vec_moves:
        mv.sent()
    for cp in stores:
        cp.wait()


def run_intake(xt, gt, wq, wo, wup, wdown, vecs, cid):
    copies = PEERS - 1 + 3 * GATHER_COPIES
    bufs = [jax.ShapeDtypeStruct((PEERS, n * ROWS, D), BF16) for n in (3, 1) + (2,) * DEPTH]
    vmem = pltpu.VMEM
    return pl.pallas_call(
        intake_kernel,
        in_specs=[ANY] * 6 + [pl.BlockSpec(memory_space=vmem)],
        out_specs=[pl.BlockSpec(memory_space=vmem)] * 2 + [ANY] * len(bufs) + [pl.BlockSpec(memory_space=vmem)],
        out_shape=[act(), act()] + bufs + [f32s(16, D)],
        scratch_shapes=[vmem((2, SEQ, NSEQ, D), BF16), vmem((PEERS, SEQ * NSEQ, LANES), F32),
                        vmem(wq.shape, F32), vmem(wo.shape, F32), vmem(wup.shape, F32), vmem(wdown.shape, F32),
                        vmem((3 * ROWS, D), BF16), vmem((DEPTH + 1, 2 * ROWS, D), BF16), vmem((PEERS, 16, LANES), F32),
                        pltpu.SemaphoreType.DMA((copies,)), pltpu.SemaphoreType.DMA((copies,)),
                        pltpu.SemaphoreType.DMA((6 + 2 + DEPTH,))],
        compiler_params=pltpu.CompilerParams(vmem_limit_bytes=VMEM_MAX, collective_id=cid, has_side_effects=True),
        name="intake",
    )(xt, gt, wq, wo, wup, wdown, vecs)


def qkv_kernel(traffic, x_ref, wq_ref, wk_ref, wv_ref, vec_ref, *refs):
    n_in, n_out, _ = traffic.sizes()
    srcs, (h_ref, q_ref, k_ref, v_ref, *refs) = refs[:n_in], refs[n_in:]
    i = pl.program_id(0)
    traffic.begin(i, srcs, refs[:n_out], refs[n_out:])
    rows = x_ref.shape[0] * PAD
    g1, c1, *_ = table_rows(vec_ref)
    xhat, _ = ln_fwd(x_ref[:].reshape(rows, D).astype(F32))
    h = (xhat * g1 + c1).astype(BF16)
    h_ref[:] = h.reshape(h_ref.shape)
    biases = table_rows(vec_ref, V_QKV, 3)
    for w_ref, o_ref, bias in zip((wq_ref, wk_ref, wv_ref), (q_ref, k_ref, v_ref), biases):
        o_ref[:] = (dot_nn(h, w_ref[:].reshape(D, D)) + bias).astype(BF16).reshape(o_ref.shape)
    traffic.finish(i == pl.num_programs(0) - 1)


def run_qkv(xp, wall, vec, cid, items):
    bs = 2
    traffic = Traffic(items)
    tok = pl.BlockSpec((bs, PAD, D), lambda s: (s, 0, 0))
    outs = pl.pallas_call(
        functools.partial(qkv_kernel, traffic), grid=(NSEQ // bs,),
        in_specs=[tok, *map(wblk, range(3)), fixed(vec.shape)] + traffic.in_specs(),
        out_specs=[tok] * 4 + traffic.out_specs(), out_shape=[act()] * 4 + traffic.out_shapes(),
        scratch_shapes=traffic.scratch(), input_output_aliases=traffic.aliases(5, 4),
        compiler_params=comm_params(cid), name="qkv",
    )(xp, wall, wall, wall, vec, *traffic.arrays())
    return outs[:4], traffic.split(outs[4:])


def low_lanes(rows):
    return lax.broadcasted_iota(jnp.int32, (rows, LANES), 1) < HEAD


def keys_mask(st):
    tail = st[MAIN:PAD]
    row = lax.broadcasted_iota(jnp.int32, tail.shape, 0)
    return jnp.concatenate([st[:MAIN], jnp.where(row < SEQ - MAIN, tail, NEG)], axis=0)


def diag_mask(heads):
    shape = (heads, heads * HEAD)
    row = lax.broadcasted_iota(jnp.int32, shape, 0)
    return lax.broadcasted_iota(jnp.int32, shape, 1) // HEAD == row


def last_by_head(t_ref, dmask, cols=slice(None)):
    last = t_ref[MAIN:PAD, cols][:1]
    return jnp.where(dmask, jnp.broadcast_to(last.astype(F32), dmask.shape), 0.0).astype(BF16)


def only_first_row(t):
    row = lax.broadcasted_iota(jnp.int32, (TAIL, t.shape[1]), 0)
    return jnp.where(row == 0, jnp.broadcast_to(t, row.shape), 0.0)


def softmax_t(st):
    st = keys_mask(st)
    m = jnp.max(st, axis=0, keepdims=True) * (SCALE * LOG2E)
    e = jnp.exp2(st * (SCALE * LOG2E) - m)
    total = col_sum(e)
    return e, total, m


def two_heads(t, low):
    zero = jnp.zeros(t.shape, t.dtype)
    return jnp.where(low, t, zero), jnp.where(low, zero, t)


def attn_fwd_kernel(traffic, q_ref, k_ref, v_ref, x_ref, g_ref, wo_ref, vec_ref, *refs):
    n_in, n_out, _ = traffic.sizes()
    srcs, (o_ref, a_ref, y_ref, h2_ref, dm_ref, lse_ref, *refs) = refs[:n_in], refs[n_in:]
    dsts, (s_s, p_s, *rest) = refs[:n_out], refs[n_out:]
    i = pl.program_id(0)
    traffic.begin(i, srcs, dsts, rest)
    low_q = low_lanes(MAIN)
    for p in range(HEADS // 2):
        halves = two_heads(q_ref[:MAIN, block(p)], low_q)
        for hh, qa in enumerate(halves):
            s_s[2 * p + hh] = dot_nt(k_ref[:, block(p)], qa)

    @pl.loop(0, ONCE)
    def _(t):
        for h in range(HEADS):
            e, total, m = softmax_t(s_s[h])
            p_s[h] = (e * (1.0 / total)).astype(BF16)
            lse_ref[h:h + 1, :] = m + jnp.log(total) * LOG2E

    for p in range(HEADS // 2):
        vt = v_ref[:, block(p)].T
        outs = [dot_nn(vt[hh * HEAD:(hh + 1) * HEAD], p_s[2 * p + hh]) for hh in range(2)]
        o_ref[:MAIN, block(p)] = jnp.concatenate(outs, axis=0).astype(BF16).T
    dmask = diag_mask(HEADS)
    e, total, _ = softmax_t(dot_nt(k_ref[:], last_by_head(q_ref, dmask)))
    ot = dot_tn((e * (1.0 / total)).astype(BF16), v_ref[:])
    o_ref[MAIN:PAD] = only_first_row(col_sum(jnp.where(dmask, ot, 0.0))).astype(BF16)

    _, _, bo, s1, g2, c2, _, s2 = table_rows(vec_ref)
    a = dot_nn(o_ref[:], wo_ref[:].reshape(D, D)) + bo
    a_ref[:] = a
    y = x_ref[:].astype(F32) + s1 * a
    y_ref[:] = y
    xhat, _ = ln_fwd(y)
    h2_ref[:] = (xhat * g2 + c2).astype(BF16)
    dm_ref[:] = (g_ref[:].astype(F32) * s2).astype(BF16)
    traffic.finish(i == NSEQ - 1)


def run_attn_fwd(q, k, v, xp, gp, wo, vec, cid, items):
    traffic = Traffic(items)
    tok = one_seq()
    outs = pl.pallas_call(
        functools.partial(attn_fwd_kernel, traffic), grid=(NSEQ,),
        in_specs=[tok] * 5 + [wblk(0), fixed(vec.shape)] + traffic.in_specs(),
        out_specs=[tok] * 5 + [pl.BlockSpec((None, HEADS, MAIN), lambda s: (s, 0, 0))] + traffic.out_specs(),
        out_shape=[act(), act(dtype=F32), act(dtype=F32), act(), act(), f32s(NSEQ, HEADS, MAIN)] + traffic.out_shapes(),
        scratch_shapes=[pltpu.VMEM((HEADS, PAD, MAIN), F32), pltpu.VMEM((HEADS, PAD, MAIN), BF16)] + traffic.scratch(),
        input_output_aliases=traffic.aliases(7, 6),
        compiler_params=comm_params(cid), name="attn_fwd",
    )(q, k, v, xp, gp, wo, vec, *traffic.arrays())
    return outs[:6], traffic.split(outs[6:])


def owner_rows(load, core):
    _, y, x, _ = coords()
    pieces = []
    for yy in (y, 1 - y):
        for xx in (x, 1 - x):
            pieces.append(load(pl.ds(pl.multiple_of((4 * yy + 2 * xx + core) * ROWS, ROWS), ROWS)))
    return jnp.concatenate(pieces, axis=1)


def store_piece(ab_ref, mine_ref, came_ref, unit):
    for color in range(2):
        for ry in range(2):
            for rx in range(2):
                r = 2 * ry + rx
                rows = slice(r * ROWS, (r + 1) * ROWS)
                sent, pos = (rx, ry) if color == 0 else (ry, rx)
                ab_ref[color, sent, pos, unit] = mine_ref[color, rows] + came_ref[color, rows]


class CorePair:
    def __init__(self, i, order, part_s, recv_s, sems):
        self.i, self.order, self.part_s, self.recv_s = i, order, part_s, recv_s
        self.slots = part_s.shape[0]
        self.sends = [[Move(remote(part_s.at[u % self.slots, n], recv_s.at[u, n], sems, 2 * u + n, partner("core")))
                       for n in range(2)] for u in range(recv_s.shape[0])]

    def before(self):
        for step, (what, u) in self.order.items():
            @pl.when(self.i == step)
            def _(step=step, what=what, u=u):
                came, prev = self.order.get(step - 1, ("none", 0))
                if came == "part":
                    self.sends[prev][1].start()
                if what == "mine":
                    for mv in self.sends[u]:
                        mv.sent()

    def product(self, u, left, right):
        theirs, mine = [next(st for st, which in self.order.items() if which == (what, u)) for what in ("part", "mine")]
        core = lax.rem(lax.axis_index("fsdp"), 2)

        @pl.when((self.i == theirs) | (self.i == mine))
        def _():
            who = jnp.where(self.i == mine, core, 1 - core)

            @pl.loop(0, 2)
            def _(n):
                @pl.when((self.i == theirs) & (n == 1))
                def _():
                    self.sends[u][0].start()
                cols = pl.ds(pl.multiple_of(n * HD, HD), HD)
                self.part_s[u % self.slots, n] = dot_tn(owner_rows(left, who), right(cols))

    def after(self, ab_ref, unit_of):
        for step, (what, u) in self.order.items():
            if what == "mine":
                @pl.when(self.i == step)
                def _(u=u):
                    for mv in self.sends[u]:
                        mv.recv()
                    store_piece(ab_ref, self.part_s.at[u % self.slots], self.recv_s.at[u], unit_of(u))


def pair_scratch(n):
    half = (2, 4 * ROWS, HD)
    return [pltpu.VMEM((2,) + half, F32), pltpu.VMEM((n,) + half, F32),
            pltpu.SemaphoreType.DMA((2 * n,)), pltpu.SemaphoreType.DMA((2 * n,))]


def piece_spec(width, n, before):
    return pl.BlockSpec((2, 2, 2, 1, ROWS, width // 2),
                        lambda i: (0, 0, 0, jnp.clip(i - before, 0, n - 1), 0, 0))


def mlp_kernel(first, traffic, h2_any, dm_any, wff_any, b1_ref, *refs):
    n_in, n_out, _ = traffic.sizes()
    if not first:
        m_in, dh_in, *refs = refs
    srcs, (m_out, dh_out, ab_ref, db_ref, *refs) = refs[:n_in], refs[n_in:]
    dsts, (h2_ref, dm_ref, w_s, load_sem, act_s, du_s, part_s, recv_s, core_send, core_recv, *rest) = refs[:n_out], refs[n_out:]
    i = pl.program_id(0)
    bs = m_out.shape[0]
    rows = bs * PAD
    nblk = NSEQ // bs
    traffic.begin(i, srcs, dsts, rest)

    loads = [pltpu.make_async_copy(wff_any.at[:, block(k)], w_s.at[k], load_sem.at[k]) for k in range(2)]
    w1_load, w2_load = loads

    def blocks(j):
        some = pl.ds(j * bs, bs)
        return [pltpu.make_async_copy(src.at[some], dst.at[some], load_sem.at[2 + 2 * j + k])
                for k, (src, dst) in enumerate(((h2_any, h2_ref), (dm_any, dm_ref)))]

    @pl.when(i == 0)
    def _():
        db_ref[:] = jnp.zeros_like(db_ref)
        h2_load, dm_load = blocks(0)
        for cp in (w1_load, h2_load, w2_load, dm_load):
            cp.start()
        for j in range(1, nblk):
            for cp in blocks(j):
                cp.start()

    for j in range(nblk):
        @pl.when(i == j)
        def _(j=j):
            for cp in blocks(j) + ([] if j else loads):
                cp.wait()

    @pl.when(i < nblk)
    def _():
        hb = h2_ref[pl.ds(i * bs, bs)].reshape(rows, D)
        dmb = dm_ref[pl.ds(i * bs, bs)].reshape(rows, D)
        w1 = w_s[0].reshape(D, QTR)
        w2 = w_s[1].reshape(QTR, D)
        mine = pl.ds(pl.multiple_of(i * rows, rows), rows)
        cw = 2 * LANES
        for c in range(QTR // cw):
            cols = slice(c * cw, (c + 1) * cw)
            u = dot_nn(hb, w1[:, cols]) + b1_ref[:, cols]
            da = dot_nt(dmb, w2[cols])
            cdf = 0.5 + 0.5 * lax.erf(u * (0.5 ** 0.5))
            slope = cdf + u * (jnp.exp(-0.5 * u * u) * 0.3989422804014327)
            du = da * slope
            db_ref[:, cols] += sub8(du)
            act_s[mine, cols] = (u * cdf).astype(BF16)
            du_s[mine, cols] = du.astype(BF16)
        m = dot_nn(act_s[mine, :], w2).reshape(m_out.shape)
        dh = dot_nt(du_s[mine, :], w1).reshape(dh_out.shape)
        m_out[:] = m if first else m_in[:] + m
        dh_out[:] = dh if first else dh_in[:] + dh

    flat = NSEQ * PAD
    order = {nblk + 2 * k + u: (what, u) for k, what in enumerate(("part", "mine")) for u in range(2)}
    pair = CorePair(i, order, part_s, recv_s, (core_send, core_recv))
    pair.before()
    pair.product(0, lambda lanes: h2_ref[:, :, lanes].reshape(flat, ROWS), lambda cols: du_s[:, cols])
    pair.product(1, lambda lanes: act_s[:, lanes], lambda cols: dm_ref[:, :, cols].reshape(flat, cols.size))
    pair.after(ab_ref, lambda u: 0)
    traffic.finish(i == pl.num_programs(0) - 1)


def run_mlp(h2, dm, wff, b1, acc, cid, items=()):
    traffic = Traffic(items, ("core",))
    bs = 2
    nblk = NSEQ // bs
    tok = pl.BlockSpec((bs, PAD, D), lambda i: (jnp.minimum(i, nblk - 1), 0, 0))
    args = (h2, dm, wff, b1) + acc
    base = len(args)
    outs = pl.pallas_call(
        functools.partial(mlp_kernel, not acc, traffic), grid=(nblk + 4,),
        in_specs=[ANY] * 3 + [fixed(b1.shape)] + [tok] * len(acc) + traffic.in_specs(),
        out_specs=[tok, tok, piece_spec(D, 2, nblk + 2), resident((8, QTR))] + traffic.out_specs(),
        out_shape=[act(dtype=F32), act(dtype=F32), f32s(2, 2, 2, 2, ROWS, HD), f32s(8, QTR)] + traffic.out_shapes(),
        scratch_shapes=[pltpu.VMEM(h2.shape, BF16), pltpu.VMEM(dm.shape, BF16), pltpu.VMEM((2, PEERS, ROWS, D), BF16),
                        pltpu.SemaphoreType.DMA((2 + 2 * nblk,))] + [pltpu.VMEM((NSEQ * PAD, QTR), BF16)] * 2
        + pair_scratch(2) + traffic.scratch(),
        input_output_aliases={**{base - len(acc) + k: k for k in range(len(acc))}, **traffic.aliases(base, 4)},
        compiler_params=comm_params(cid), name="mlp",
    )(*args, *traffic.arrays())
    m, dh, ab, db, *rest = outs
    return (m, dh), ab, db, traffic.split(rest)


ORDER = ("part0", "part1", "mine0", "part2", "mine1", "part3", "mine2", "mine3")
EARLY = 2
LOADED = ("o", "da", "h1", "dv", "dk", "dq")
LOADED_AT = ("o da", "h1 dv", "", "dk", "", "dq")


def wgrad_kernel(traffic, *refs):
    given, refs = refs[:len(LOADED)], refs[len(LOADED):]
    n_in, n_out, _ = traffic.sizes()
    srcs, (ab_ref, *refs) = refs[:n_in], refs[n_in:]
    early, refs = refs[:EARLY], refs[EARLY:]
    dsts, refs = refs[:n_out], refs[n_out:]
    here, refs = refs[:len(LOADED)], refs[len(LOADED):]
    load_sem, part_s, recv_s, core_send, core_recv, s1_send, s1_recv, *rest = refs
    i = pl.program_id(0)
    flat = NSEQ * PAD
    traffic.begin(i, srcs, dsts, rest)
    loads = [pltpu.make_async_copy(src, dst, load_sem.at[k]) for k, (src, dst) in enumerate(zip(given, here))]

    @pl.when(i == 0)
    def _():
        for cp in loads:
            cp.start()

    for step, some in enumerate(LOADED_AT):
        @pl.when(i == step)
        def _(some=some):
            for name in some.split():
                loads[LOADED.index(name)].wait()

    o, da, h1, dv, dk, dq = here
    units = ((o, da), (h1, dv), (h1, dk), (h1, dq))
    onward = [[Move(remote(ab_ref.at[color, 1, :, u], got.at[color], (s1_send, s1_recv), 2 * u + color, partner(nm)))
               for color, nm in enumerate(NAMES["s1"])] for u, got in enumerate(early)]
    order = {step: (name[:DEPTH], int(name[DEPTH:])) for step, name in enumerate(ORDER)}
    pair = CorePair(i, order, part_s, recv_s, (core_send, core_recv))
    pair.before()
    for step, (what, u) in order.items():
        if what == "mine" and u < EARLY:
            @pl.when(i == step + 1)
            def _(u=u):
                for mv in onward[u]:
                    mv.start()
    for u, (left, right) in enumerate(units):
        pair.product(u, lambda lanes, left=left: left[:, :, lanes].reshape(flat, ROWS),
                     lambda cols, right=right: right[:, :, cols].reshape(flat, cols.size))
    pair.after(ab_ref, lambda u: u)

    @pl.when(i == len(ORDER) - 1)
    def _():
        for moves in onward:
            for mv in moves:
                mv.recv()
                mv.sent()

    traffic.finish(i == len(ORDER) - 1)


def run_wgrad(ops, cid, items):
    traffic = Traffic(items, ("core", "x", "y"))
    n = DEPTH
    piece = (2, 2, 2, n, ROWS, HD)
    dma = pltpu.SemaphoreType.DMA
    outs = pl.pallas_call(
        functools.partial(wgrad_kernel, traffic), grid=(len(ORDER),),
        in_specs=[ANY] * len(ops) + traffic.in_specs(),
        out_specs=[fixed(piece)] + [ANY] * EARLY + traffic.out_specs(),
        out_shape=[f32s(*piece)] + [f32s(2, 2, ROWS, HD)] * EARLY + traffic.out_shapes(),
        scratch_shapes=[pltpu.VMEM(t.shape, BF16) for t in ops] + [dma((len(ops),))] + pair_scratch(n)
        + [dma((2 * EARLY,)), dma((2 * EARLY,))] + traffic.scratch(),
        input_output_aliases=traffic.aliases(len(ops), 1 + EARLY),
        compiler_params=comm_params(cid), name="wgrad",
    )(*ops, *traffic.arrays())
    ab, *outs = outs
    return ab, outs[:EARLY], traffic.split(outs[EARLY:])


def heads_bwd(half, q_ref, k_ref, v_ref, do_ref, lse_ref, dq_ref, dk_ref, dv_ref, sum_ref,
              dk_s, dv_s, s_s, dp_s, p_s, ds_s):
    low_q, low_k = low_lanes(MAIN), low_lanes(PAD)
    pairs = HH // 2
    cols = slice(half * HD, (half + 1) * HD)
    for p in range(pairs):
        lanes = block(half * pairs + p)
        queries = two_heads(q_ref[:MAIN, lanes], low_q)
        cots = two_heads(do_ref[:MAIN, lanes], low_q)
        for hh in range(2):
            s_s[2 * p + hh] = dot_nt(k_ref[:, lanes], queries[hh])
            dp_s[2 * p + hh] = dot_nt(v_ref[:, lanes], cots[hh])

    @pl.loop(0, ONCE)
    def _(t):
        for h in range(HH):
            dpt = dp_s[h]
            lse = lse_ref[half * HH + h:half * HH + h + 1, :]
            prob = jnp.exp2(keys_mask(s_s[h]) * (SCALE * LOG2E) - lse)
            p_s[h] = prob.astype(BF16)
            ds_s[h] = (prob * (dpt - col_sum(prob * dpt)) * SCALE).astype(BF16)

    dmask = diag_mask(HH)
    qb, dob = last_by_head(q_ref, dmask, cols), last_by_head(do_ref, dmask, cols)
    e, total, _ = softmax_t(dot_nt(k_ref[:, cols], qb))
    prob = e * (1.0 / total)
    dp = dot_nt(v_ref[:, cols], dob)
    ds = (prob * (dp - col_sum(prob * dp)) * SCALE).astype(BF16)
    dv_s[:] = dot_nn(prob.astype(BF16), dob)
    dk_s[:] = dot_nn(ds, qb)
    dq_tail = only_first_row(col_sum(jnp.where(dmask, dot_tn(ds, k_ref[:, cols]), 0.0)))
    dq_ref[MAIN:PAD, cols] = dq_tail.astype(BF16)
    sum_ref[0, :, cols] += sub8(dq_tail)

    for p in range(pairs):
        lanes = block(half * pairs + p)
        q2, do2 = q_ref[:MAIN, lanes], do_ref[:MAIN, lanes]
        kt = k_ref[:, lanes].T
        heads = range(2 * p, 2 * p + 2)
        dv = jnp.where(low_k, *[dot_nn(p_s[h], do2) for h in heads]) + dv_s[:, block(p)]
        dk = jnp.where(low_k, *[dot_nn(ds_s[h], q2) for h in heads]) + dk_s[:, block(p)]
        dq = jnp.concatenate([dot_nn(kt[hh * HEAD:(hh + 1) * HEAD], ds_s[h]) for hh, h in enumerate(heads)], axis=0).T
        dv_ref[:, lanes] = dv.astype(BF16)
        dk_ref[:, lanes] = dk.astype(BF16)
        dq_ref[:MAIN, lanes] = dq.astype(BF16)
        for k, t in enumerate((dq, dk, dv)):
            sum_ref[k, :, lanes] += sub8(t)


def heads_scratch():
    scores = (HH, PAD, MAIN)
    return [pltpu.VMEM((PAD, HD), F32), pltpu.VMEM((PAD, HD), F32), pltpu.VMEM(scores, F32), pltpu.VMEM(scores, F32),
            pltpu.VMEM(scores, BF16), pltpu.VMEM(scores, BF16)]


def back_kernel(traffic, m_ref, y_ref, dh_ref, a_ref, g_ref, q_ref, k_ref, v_ref, lse_ref, wo_ref, vec_ref, *refs):
    n_in, n_out, _ = traffic.sizes()
    srcs, (z_ref, gres_ref, da_ref, dq_ref, dk_ref, dv_ref, sum_ref, hsum_ref, *refs) = refs[:n_in], refs[n_in:]
    dsts, (do_s, *refs) = refs[:n_out], refs[n_out:]
    n = len(heads_scratch())
    heads = refs[:n]
    i = pl.program_id(0)
    traffic.begin(i, srcs, dsts, refs[n:])

    @pl.when(i == 0)
    def _():
        sum_ref[:] = jnp.zeros_like(sum_ref)
        hsum_ref[:] = jnp.zeros_like(hsum_ref)

    _, _, _, s1, g2, _, b2, s2 = table_rows(vec_ref)
    g = g_ref[:].astype(F32)
    y = y_ref[:]
    m = m_ref[:] + b2
    z_ref[:] = (y + s2 * m).astype(BF16)[:SEQ]
    dh = dh_ref[:]
    xhat, rstd = ln_fwd(y)
    gres = g + ln_bwd(dh * g2, xhat, rstd)
    gres_ref[:] = gres
    da = gres * s1
    for k, t in enumerate((da, gres * a_ref[:], dh * xhat, dh, g * s2, g * m)):
        sum_ref[k] += sub8(t)
    dab = da.astype(BF16)
    da_ref[:] = dab
    do_s[:] = dot_nt(dab, wo_ref[:].reshape(D, D)).astype(BF16)
    for half in range(2):
        heads_bwd(half, q_ref, k_ref, v_ref, do_s, lse_ref, dq_ref, dk_ref, dv_ref, hsum_ref, *heads)
    traffic.finish(i == NSEQ - 1)


def run_back(m, y, dh, a, gp, q, k, v, lse, wo, vec, cid, items):
    traffic = Traffic(items)
    tok = one_seq()
    outs = pl.pallas_call(
        functools.partial(back_kernel, traffic), grid=(NSEQ,),
        in_specs=[tok] * 8 + [pl.BlockSpec((None, HEADS, MAIN), lambda s: (s, 0, 0)), wblk(0), fixed(vec.shape)]
        + traffic.in_specs(),
        out_specs=[pl.BlockSpec((None, SEQ, D), lambda s: (s, 0, 0))] + [tok] * 5
        + [resident((6, 8, D)), resident((3, 8, D))] + traffic.out_specs(),
        out_shape=[jax.ShapeDtypeStruct((NSEQ, SEQ, D), BF16), act(dtype=F32)] + [act()] * 4
        + [f32s(6, 8, D), f32s(3, 8, D)] + traffic.out_shapes(),
        scratch_shapes=[pltpu.VMEM((PAD, D), BF16)] + heads_scratch() + traffic.scratch(),
        input_output_aliases=traffic.aliases(11, 8),
        compiler_params=comm_params(cid), name="back",
    )(m, y, dh, a, gp, q, k, v, lse, wo, vec, *traffic.arrays())
    return outs[:8], traffic.split(outs[8:])


def adds_kernel(n, *refs):
    ins, outs = refs[:2 * n], refs[2 * n:]
    for a_ref, b_ref, o_ref in zip(ins[::2], ins[1::2], outs):
        o_ref[:] = a_ref[:].reshape(o_ref.shape) + b_ref[:].reshape(o_ref.shape)


def quarters(shape, kept=False):
    *lead, rows, width = shape
    lead = (1,) + ((1,) + tuple(lead[2:]) if kept else tuple(lead[1:]))
    zeros = (0,) * (len(lead) - 1)
    return pl.BlockSpec(lead + (rows // 2, width), lambda g: (g // 2,) + zeros + (lax.rem(g, 2), 0))


def run_adds(*jobs):
    specs, outs = [], []
    for a, b in jobs:
        outs.append(quarters(b.shape))
        specs += [quarters(a.shape, a.ndim > b.ndim), outs[-1]]
    return pl.pallas_call(
        functools.partial(adds_kernel, len(jobs)), grid=(4,), in_specs=specs, out_specs=outs,
        out_shape=[f32s(*b.shape) for _, b in jobs],
        compiler_params=params(), name="adds",
    )(*[t for job in jobs for t in job])


def store_ff(gup_ref, gdown_ref, f_ref, j):
    half = PEERS // 2
    for k in range(PEERS):
        gup_ref[:, block(DEPTH * k + j)] = f_ref[k // half, 0, :, block(k % half)]
    for color in range(2):
        gdown_ref[j * ROWS:(j + 1) * ROWS, color * HD:(color + 1) * HD] = f_ref[color, 1]


UNITS = DEPTH
EVENTS = ("", "", "b0", "b1", "p00", "p01", "a2 p10 q00", "p11 q01")


def finish_kernel(x_ref, gres_ref, dq_ref, dk_ref, dv_ref, wq_ref, wk_ref, wv_ref, vec_ref, ab_any, keep_ref, e0, e1,
                  f0, f1, f2, p3_ref, b3_ref, sum_ref, hsum_ref, db0, db1, db2, db3,
                  dx_ref, gqkv_ref, gout_ref, gup_ref, gdown_ref, small_ref,
                  dx_s, ln_s, sk, r2, ra, rb, f3_s, small_s, all_p, part_s, all_z, ssem, rsem):
    i = pl.program_id(0)
    z, me = lax.axis_index("rep"), lax.axis_index("fsdp")
    sems, used = (ssem, rsem), []
    colors = range(2)

    def move(src, dst, device, *roles):
        used.append(Move(remote(src, dst, sems, len(used), device), *roles))
        return used[-1]

    s1 = {u: [move(ab_any.at[color, 1, :, u], sk.at[u, color], partner(nm)) for color, nm in enumerate(NAMES["s1"])]
          for u in range(EARLY, UNITS)}
    s2 = [[move(sk.at[u, color, 1], r2.at[u, color], partner(nm)) for color, nm in enumerate(NAMES["s2"])]
          for u in range(UNITS)]
    near, far = partner("near"), partner("far")
    z_a = [[move(sk.at[u, c, 0], ra.at[u, c], near, *ROLES["zA"]) for c in colors] for u in range(UNITS)]
    z_b = [[move(ra.at[u, c], rb.at[u, c], far, *ROLES["zB"]) for c in colors] for u in range(UNITS)]
    z_c = [[move(rb.at[u, c], rb.at[u, c], near, *ROLES["zC"]) for c in colors] for u in range(UNITS)]
    f3_c = move(f3_s, f3_s, near, *ROLES["zC"])
    others = [(z, lax.rem(me + k, PEERS)) for k in range(1, PEERS)]
    column = [(lax.rem(z + k, DEPTH), me) for k in range(1, DEPTH)]
    plane_moves = [move(small_s.at[to], all_p.at[me], (zz, to)) for zz, to in others]
    column_moves = [move(part_s, all_z.at[z], dev) for dev in column]

    def start(moves):
        for mv in moves:
            mv.start()

    def arrive(moves):
        for mv in moves:
            mv.recv()

    def inner(do):
        pl.when(is_inner() == 1)(do)

    def after_s1(u, came=None):
        if came is None:
            arrive(s1[u])
        for pos in (1, 0):
            for c in colors:
                got = sk[u, c, pos] if came is None else came[c, pos]
                sk[u, c, pos] = got + keep_ref[c, 0, pos, u]
        start(s2[u])

    def after_s2(u):
        arrive(s2[u])
        for c in colors:
            sk[u, c, 0] = sk[u, c, 0] + r2[u, c]
        start(z_a[u])

    def after_za(u, c):
        arrive([z_a[u][c]])

        @inner
        def _():
            ra[u, c] = ra[u, c] + sk[u, c, 0]
        start([z_b[u][c]])

    def after_zb(u, c):
        arrive([z_b[u][c]])

        @inner
        def _():
            rb[u, c] = rb[u, c] + ra[u, c]
        start([z_c[u][c]])

    @pl.when(i == 0)
    def _():
        greet(others + column)
        ln_s[:] = jnp.zeros_like(ln_s)

        @inner
        def _():
            f3_s[:] = p3_ref[:] + b3_ref[:]
        start([f3_c])
        for u, came in enumerate((e0, e1)):
            after_s1(u, came)
        for u in s1:
            start(s1[u])

    act_on = {"a": after_s1, "b": after_s2, "p": after_za, "q": after_zb}

    def handle(events):
        for kind, *which in events.split():
            act_on[kind](*map(int, which))

    for step, events in enumerate(EVENTS):
        @pl.when(i == step)
        def _(events=events):
            handle(events)

    dh = None
    for d_ref, w_ref in ((dq_ref, wq_ref), (dk_ref, wk_ref), (dv_ref, wv_ref)):
        part = dot_nt(d_ref[:], w_ref[:].reshape(D, D))
        dh = part if dh is None else dh + part
    g1, *_ = table_rows(vec_ref)
    xhat, rstd = ln_fwd(x_ref[:].astype(F32))
    for k, t in enumerate((dh * xhat, dh)):
        ln_s[k] += sub8(t)
    dx = gres_ref[:] + ln_bwd(dh * g1, xhat, rstd)
    for k in range(PEERS):
        dx_s[k, pl.ds(i, SEQ, stride=NSEQ), :] = dx[:SEQ, block(k)]

    @pl.when(i == NSEQ - 1)
    def _():
        rows = [col_sum(ref[k]) for ref in (ln_s, sum_ref) for k in range(ref.shape[0])]
        rows += [col_sum(ref[:]) for ref in (db0, db1, db2, db3)]
        blocks = [col_sum(hsum_ref[t])[:, block(k)] for t in range(3) for k in range(PEERS)]
        for to in range(PEERS):
            mine = [row[:, block(to)] for row in rows] + blocks[3 * to:3 * to + 3] + [jnp.zeros((1, LANES), F32)]
            small_s[to] = jnp.concatenate(mine, axis=0)
        start(plane_moves)
        all_p[me] = small_s[me]
        handle("a3")
        for k in range(PEERS):
            dx_ref[:, :, block(k)] = dx_s[k].reshape(SEQ, NSEQ, LANES).astype(BF16)
        handle("q10")
        arrive(plane_moves)
        part_s[:] = jnp.sum(all_p[:], axis=0)
        all_z[z] = part_s[:]
        start(column_moves)
        handle("b2 q11")
        for j, f_ref in enumerate((f0, f1, f2)):
            store_ff(gup_ref, gdown_ref, f_ref, j)
        handle("b3 p20")
        arrive([f3_c])
        store_ff(gup_ref, gdown_ref, f3_s, 3)
        arrive(column_moves)
        small_ref[:] = jnp.sum(all_z[:], axis=0)
        handle("p21 q20 p30")
        handle("q21 p31 q30 q31")
        for u, (out_ref, base) in enumerate(((gout_ref, 0), (gqkv_ref, 2 * D), (gqkv_ref, D), (gqkv_ref, 0))):
            for c in colors:
                arrive(z_c[u][c:c + 1])
                out_ref[:, base + c * HD:base + (c + 1) * HD] = rb[u, c]
        for mv in used:
            mv.sent()


def run_finish(xp, gres, grads, wall, vec, ab, early, ffs, last, sums, hsum, dbs, cid):
    tok = one_seq()
    outs = [(SEQ, NSEQ, D), (ROWS, 3 * D), (ROWS, D), (ROWS, DEPTH * D), (DEPTH * ROWS, D), (16, LANES)]

    def piece(*lead):
        return pltpu.VMEM(lead + (ROWS, HD), F32)

    scratch = [pltpu.VMEM((PEERS, SEQ * NSEQ, LANES), F32), pltpu.VMEM((2, 8, D), F32)]
    scratch += [piece(UNITS, 2, 2)] + [piece(UNITS, 2)] * 3 + [piece(2, 2)]
    scratch += [pltpu.VMEM((PEERS, 16, LANES), F32)] * 2
    scratch += [pltpu.VMEM((16, LANES), F32), pltpu.VMEM((DEPTH, 16, LANES), F32)]
    scratch += [pltpu.SemaphoreType.DMA((64,)), pltpu.SemaphoreType.DMA((64,))]
    consts = [sums, hsum] + list(dbs)
    held = [*early, *ffs, *last]
    before = [xp, gres, *grads, wall, wall, wall, vec, ab, ab, *held]
    return pl.pallas_call(
        finish_kernel, grid=(NSEQ,),
        in_specs=[tok] * 5 + [*map(wblk, range(3)), fixed(vec.shape), ANY, kept_spec(ab.shape)]
        + [fixed(t.shape) for t in held + consts],
        out_specs=[fixed(sh) for sh in outs],
        out_shape=[jax.ShapeDtypeStruct(outs[0], BF16)] + [f32s(*sh) for sh in outs[1:]],
        scratch_shapes=scratch, compiler_params=comm_params(cid), name="finish",
    )(*before, *consts)


def device_step(x_loc, dz_loc, w_qkv, b_qkv, w_out, w_up, b_up, w_down, vec_params):
    cid = itertools.count()
    vecs = jnp.concatenate([vec_params, b_up.reshape(-1, LANES), b_qkv.reshape(-1, LANES), jnp.zeros((1, LANES), F32)])
    xp, gp, wall, wo, c0, c1, c2, c3, vec = run_intake(
        x_loc.swapaxes(0, 1), dz_loc.swapaxes(0, 1), w_qkv, w_out, w_up, w_down, vecs, next(cid))
    b1 = [vec[V_UP + j:V_UP + j + 1] for j in range(DEPTH)]
    own, rest = range(2)
    (h1, q, k, v), (wo,) = run_qkv(xp, wall, vec, next(cid), [Gather(wo, own, 2, 3)])
    (o, a, y, h2, dm, lse), (c0, c1) = run_attn_fwd(
        q, k, v, xp, gp, wo, vec, next(cid), [Gather(c0, own, 3, 5), Gather(c1, own, start=3)])

    mlp = functools.partial(run_mlp, h2, dm)
    acc, f0, db0, (c1, c2, c3) = mlp(c0, b1[0], (), next(cid), [Gather(c1, rest, 3), Gather(c2, own), Gather(c3, own)])
    acc, f1, db1, (c2, c3, r0) = mlp(
        c1, b1[1], acc, next(cid), [Gather(c2, rest, 3), Gather(c3, rest, 4), Chain(f0, "s1")])
    f0, = run_adds((f0, r0))
    acc, f2, db2, (r0, r1) = mlp(c2, b1[2], acc, next(cid), [Chain(f0, "s2", ("zA", 2)), Chain(f1, "s1")])
    f1, f0 = run_adds((f1, r1), r0)
    acc, f3, db3, (r1, r2, r0) = mlp(
        c3, b1[3], acc, next(cid), [Chain(f1, "s2", ("zA", 2)), Chain(f2, "s1"), Chain(f0, "zB")])
    f2, f1, f0 = run_adds((f2, r2), r1, (f0, r0))
    m, dh = acc
    (z, gres, da, dq, dk, dv, sums, hsum), (r2, r3, f1, f0) = run_back(
        m, y, dh, a, gp, q, k, v, lse, wo, vec, next(cid),
        [Chain(f2, "s2", ("zA", 2), ("zB", 4, 5)), Chain(f3, "s1", ("s2", 5)), Chain(f1, "zB", ("zC", 2, 4)), Chain(f0, "zC")])
    f3, f2 = run_adds(r3, r2)
    ab, early, (r3, f2) = run_wgrad([o, da, h1, dv, dk, dq], next(cid), [Chain(f3, "zA", ("zB", 4, 7)), Chain(f2, "zC")])
    dx, g_qkv, g_out, g_up, g_down, small = run_finish(
        xp, gres, [dq, dk, dv], wall, vec, ab, early, [f0, f1, f2], r3, sums, hsum, [db0, db1, db2, db3], next(cid))
    g_bup, g_bqkv = small[V_UP:V_QKV].reshape(-1), small[V_QKV:V_QKV + 3].reshape(-1)
    return z, dx.swapaxes(0, 1), g_qkv, g_bqkv, g_out, g_up, g_bup, g_down, small[:V_UP]


def solution(mesh):
    batch = P(("rep", "fsdp"), None, None)
    row, flat, col = P("fsdp", None), P("fsdp"), P(None, "fsdp")
    par = (row, flat, row, row, flat, row, col)
    return jax.shard_map(device_step, mesh=mesh, in_specs=(batch, batch) + par,
                         out_specs=(batch, batch) + par, check_vma=False)
```

```python
import functools
import itertools

import jax
import jax.numpy as jnp
from jax import lax
from jax.experimental import pallas as pl
from jax.experimental.pallas import tpu as pltpu
from jax.sharding import PartitionSpec as P

F32 = jnp.float32
BF16 = jnp.bfloat16
LN_EPS = 1e-5
HEADS = 16
D = 1024
SEQ = 257
NSEQ = 8
PAD = 272
MAIN = 256
TAIL = PAD - MAIN
HEAD = D // HEADS
SCALE = HEAD ** -0.5
LOG2E = 1.4426950408889634
NEG = -1e30
QTR = 1024
ROWS = 128
LANES = 128
HD = D // 2
HH = HEADS // 2
PEERS = 8
DEPTH = 4
VMEM_MAX = 62 * 1024 * 1024
MESH = pl.DeviceIdType.MESH
ANY = pl.BlockSpec(memory_space=pl.ANY)
V_UP, V_QKV = 8, 12


def dot_nn(a, b):
    return lax.dot_general(a, b, (((1,), (0,)), ((), ())), preferred_element_type=F32)


def dot_nt(a, b):
    return lax.dot_general(a, b, (((1,), (1,)), ((), ())), preferred_element_type=F32)


def dot_tn(a, b):
    return lax.dot_general(a, b, (((0,), (0,)), ((), ())), preferred_element_type=F32)


def row_mean(t):
    return jnp.mean(t, axis=-1, keepdims=True)


def col_sum(t):
    return jnp.sum(t, axis=0, keepdims=True)


def ln_fwd(t):
    cen = t - row_mean(t)
    rstd = lax.rsqrt(row_mean(cen * cen) + LN_EPS)
    return cen * rstd, rstd


def ln_bwd(dxhat, xhat, rstd):
    return rstd * (dxhat - row_mean(dxhat) - xhat * row_mean(dxhat * xhat))


def sub8(t):
    return jnp.sum(t.reshape(t.shape[0] // 8, 8, t.shape[1]), axis=0)


def table_rows(ref, first=0, count=8):
    return [ref[k:k + 1] for k in range(first, first + count)]


def block(k):
    return slice(k * LANES, (k + 1) * LANES)


def params():
    return pltpu.CompilerParams(dimension_semantics=("arbitrary",), vmem_limit_bytes=VMEM_MAX)


def comm_params(cid):
    return pltpu.CompilerParams(dimension_semantics=("arbitrary",), vmem_limit_bytes=VMEM_MAX,
                                collective_id=cid, has_side_effects=True)


def fixed(shape):
    zeros = (0,) * len(shape)
    return pl.BlockSpec(shape, lambda *_: zeros, pipeline_mode=pl.Buffered(1))


def resident(shape):
    zeros = (0,) * len(shape)
    return pl.BlockSpec(shape, lambda *_: zeros)


def wblk(i):
    return pl.BlockSpec((PEERS, ROWS, D), lambda *_: (0, i, 0), pipeline_mode=pl.Buffered(1))


def one_seq(width=D, col=0):
    return pl.BlockSpec((None, PAD, width), lambda s: (s, 0, col))


def act(width=D, dtype=BF16):
    return jax.ShapeDtypeStruct((NSEQ, PAD, width), dtype)


def f32s(*shape):
    return jax.ShapeDtypeStruct(shape, F32)


def coords():
    me, z = lax.axis_index("fsdp"), lax.axis_index("rep")
    return z, me // 4, lax.rem(me // 2, 2), lax.rem(me, 2)


def index_of(name):
    _, y, x, c = coords()
    if "core" in name:
        c = 1 - c
    if "x" in name:
        x = 1 - x
    if "y" in name:
        y = 1 - y
    return 4 * y + 2 * x + c


def partner(name):
    z = lax.axis_index("rep")
    if name == "near":
        z = z + 1 - 2 * lax.rem(z, 2)
    elif name == "far":
        z = 3 - z
    return (z, index_of(name if name in ("core", "x", "y") else ""))


def is_inner():
    z = lax.axis_index("rep")
    return lax.rem(z + z // 2, 2)


def greet(devices, extra=0):
    sem = pltpu.get_barrier_semaphore()
    for dev in devices:
        pl.semaphore_signal(sem, inc=1, device_id=dev, device_id_type=MESH)
    pl.semaphore_wait(sem, len(devices) + extra)


def barrier(names):
    far = "far" in names
    inner = is_inner()
    if far:
        @pl.when(inner == 1)
        def _():
            pl.semaphore_signal(pltpu.get_barrier_semaphore(), inc=1, device_id=partner("far"), device_id_type=MESH)
    greet([partner(name) for name in names if name != "far"], inner if far else 0)


def remote(src, dst, sems, k, device):
    send_sem, recv_sem = sems
    return pltpu.make_async_remote_copy(src_ref=src, dst_ref=dst, send_sem=send_sem.at[k], recv_sem=recv_sem.at[k],
                                        device_id=device, device_id_type=MESH)


class Move:
    def __init__(self, copy, sender="every", receiver="every"):
        self.copy, self.sender, self.receiver = copy, sender, receiver

    def role(self, who, do):
        if who == "every":
            do()
        else:
            pl.when(is_inner() == int(who == "inner"))(do)

    def start(self):
        self.role(self.sender, self.copy.start)

    def recv(self):
        self.role(self.receiver, self.copy.wait_recv)

    def sent(self):
        self.role(self.sender, self.copy.wait_send)


ROLES = {"zA": ("outer", "inner"), "zB": ("inner", "inner"), "zC": ("inner", "outer")}
NAMES = {"s1": ("x", "y"), "s2": ("y", "x"), "zA": ("near", "near"), "zB": ("far", "far"), "zC": ("near", "near"),
         "gather": ("core", "x", "y")}
GATHER_COPIES = 8
END = -1
ONCE = 1


def passes(shape):
    return shape[:1] + shape[2:] if len(shape) > 4 else shape


def kept_spec(shape):
    full = (shape[0], 1) + shape[2:] if len(shape) > 4 else shape
    zeros = (0,) * len(shape)
    return pl.BlockSpec(full, lambda *_: zeros, pipeline_mode=pl.Buffered(1))


class Chain:
    def __init__(self, array, first, *plan):
        self.array = array
        self.stages = [first] + [st for st, *_ in plan]
        self.steps = [(0, 0)] + [(steps[0], steps[-1]) for _, *steps in plan]
        self.ends = self.stages[-1] == "zC"
        self.many = len(self.stages) > 1
        self.names = [nm for st in self.stages for nm in NAMES[st]]
        self.held = []
        shape = array.shape
        for _ in plan:
            shape = passes(shape)
            self.held.append(shape)
        self.kept, self.last = passes(shape), passes(shape)

    def args(self):
        return [self.array] * (1 + self.many)

    def in_specs(self):
        return [ANY, kept_spec(self.array.shape)][:1 + self.many]

    def results(self):
        kept = [(fixed(self.kept), self.kept)] * self.many
        return kept if self.many and self.ends else kept + [(ANY, self.last)]

    def scratch(self):
        return [pltpu.VMEM(shape, F32) for shape in self.held]

    def bind(self, ins, outs, held, sems, k):
        self.kept_out = outs[0]
        sources = ins[:1] + held
        targets = held + ([held[-1]] if self.many and self.ends else outs[-1:])
        if self.ends and not self.many:
            sources = outs[-1:]
        self.sums, self.adds, self.moves = held, ins[1:] + held, []
        for st, src, dst in zip(self.stages, sources, targets):
            moves = []
            for color, name in enumerate(NAMES[st]):
                a = src.at[color, 1] if st in ("s1", "s2") else src.at[color]
                moves.append(Move(remote(a, dst.at[color], sems, k, partner(name)), *ROLES.get(st, ())))
                k += 1
            self.moves.append(moves)
        return k

    def pass_on(self, n, color):
        if n:
            self.moves[n - 1][color].recv()
            held, kept = self.sums[n - 1], self.adds[n - 1]

            def add():
                mine = kept[color, 0] if len(kept.shape) > len(held.shape) else kept[color]
                held[color] = held[color] + mine
            if self.stages[n - 1] in ROLES:
                pl.when(is_inner() == 1)(add)
            else:
                add()
        self.moves[n][color].start()

    def step(self, i):
        for n, steps in enumerate(self.steps):
            for color, step in enumerate(steps):
                @pl.when(i == step)
                def _(n=n, color=color):
                    self.pass_on(n, color)

    def finish(self):
        for mv in self.moves[-1]:
            mv.recv()
        if self.many:
            held = self.sums[-1]
            self.kept_out[:] = held[:, 0] if len(held.shape) > len(self.kept) else held[:]
        for moves in self.moves:
            for mv in moves:
                mv.sent()


class Gather:
    names = NAMES["gather"]

    def __init__(self, buf, first, *steps, start=0):
        self.buf, self.plan = buf, [(first + j, step) for j, step in enumerate((start,) + steps)]

    def args(self):
        return [self.buf]

    def in_specs(self):
        return [ANY]

    def results(self):
        return [(ANY, self.buf.shape)]

    def scratch(self):
        return []

    def bind(self, ins, outs, held, sems, k):
        self.rounds = gather_moves(outs[0], sems, k)
        return k + GATHER_COPIES

    def step(self, i):
        for j, (rnd, step) in enumerate(self.plan):
            @pl.when(i == step)
            def _(j=j, rnd=rnd):
                if j:
                    pass_on([self.rounds], rnd)
                else:
                    for mv in self.rounds[rnd].every:
                        mv.start()

    def finish(self):
        for rnd, step in self.plan:
            if step == END:
                pass_on([self.rounds], rnd)
        for j, (rnd, _) in enumerate(self.plan):
            for mv in self.rounds[rnd].kept if j + 1 < len(self.plan) else self.rounds[rnd].every:
                mv.recv()
            for mv in self.rounds[rnd].every:
                mv.sent()


class Traffic:
    def __init__(self, items=(), extra=()):
        self.items = list(items)
        self.names = sorted({nm for item in self.items for nm in item.names} | set(extra))
        self.count = sum(GATHER_COPIES if isinstance(item, Gather) else len(item.names) for item in self.items)

    def arrays(self):
        return [arr for item in self.items for arr in item.args()]

    def in_specs(self):
        return [spec for item in self.items for spec in item.in_specs()]

    def out_specs(self):
        return [spec for item in self.items for spec, _ in item.results()]

    def out_shapes(self):
        return [jax.ShapeDtypeStruct(shape, item.args()[0].dtype) for item in self.items for _, shape in item.results()]

    def scratch(self):
        n = max(self.count, 1)
        held = [each for item in self.items for each in item.scratch()]
        return held + [pltpu.SemaphoreType.DMA((n,)), pltpu.SemaphoreType.DMA((n,))]

    def sizes(self):
        return len(self.in_specs()), len(self.out_specs()), len(self.scratch())

    def aliases(self, ins, outs):
        pairs = {}
        for item in self.items:
            if isinstance(item, Gather) or (item.ends and not item.many):
                pairs[ins] = outs
            ins, outs = ins + len(item.in_specs()), outs + len(item.results())
        return pairs

    def split(self, results):
        results, out = list(results), []
        for item in self.items:
            n = len(item.results())
            out.append(results[0] if n == 1 else tuple(results[:n]))
            results = results[n:]
        return out

    def begin(self, i, ins, outs, scratch):
        ins, outs, scratch = list(ins), list(outs), list(scratch)
        *scratch, send_sem, recv_sem = scratch
        k = 0
        for item in self.items:
            n, m, h = len(item.in_specs()), len(item.results()), len(item.scratch())
            k = item.bind(ins[:n], outs[:m], scratch[:h], (send_sem, recv_sem), k)
            ins, outs, scratch = ins[n:], outs[m:], scratch[h:]
        if self.names:
            @pl.when(i == 0)
            def _():
                barrier(self.names)
        for item in self.items:
            item.step(i)

    def finish(self, last):
        if self.items:
            @pl.when(last)
            def _():
                for item in self.items:
                    item.finish()


def pass_on(gathers, rnd):
    for rounds in gathers:
        for mv in rounds[rnd - 1].passed_on:
            mv.recv()
        for mv in rounds[rnd].every:
            mv.start()


class Round:
    def __init__(self, kept, passed_on):
        self.kept, self.passed_on, self.every = kept, passed_on, kept + passed_on


def gather_moves(buf, sems, k, own=None, rows=slice(None), half=None):
    n = buf.shape[1]
    me, at_x, at_y, at_xy = index_of(""), index_of("x"), index_of("y"), index_of("xy")
    low, high = half or (slice(0, n // 2), slice(n // 2, n))

    def mv(j, src, dst, name):
        return Move(remote(src, dst, sems, k + j, partner(name)))

    mine = buf.at[me, rows]
    first = [mv(j, mine if own is None else own, mine, name) for j, name in enumerate(NAMES["gather"])]
    second = [(at_x, rows, "core"), (at_y, rows, "core"), (at_y, low, "x"), (at_x, high, "y")]
    second = [mv(len(first) + j, buf.at[who, part], buf.at[who, part], name) for j, (who, part, name) in enumerate(second)]
    last = buf.at[at_xy, rows]
    third = [mv(len(first) + len(second), last, last, "core")]
    return Round(first[:1], first[1:]), Round(second[:2], second[2:]), Round(third, [])


def intake_kernel(xt, gt, wq, wo, wup, wdown, vecs, xp_ref, gp_ref, wall, wo_buf, *refs):
    (*ff_bufs, table_ref, xs, wide, wq_s, wo_s, up_s, down_s, own, ff_own, all_v,
     ssem, rsem, lsem) = refs
    me = index_of("")
    z = lax.axis_index("rep")
    loads = [pltpu.make_async_copy(src, dst, lsem.at[k]) for k, (src, dst) in enumerate((
        (wq, wq_s), (wo, wo_s), (wup, up_s), (wdown, down_s), (xt, xs.at[0]), (gt, xs.at[1])))]
    get_wq, get_wo, get_up, get_down, get_x, get_g = loads
    for cp in loads:
        cp.start()
    greet([(z, lax.rem(me + k, PEERS)) for k in range(1, PEERS)])
    vec_moves = [Move(remote(vecs, all_v.at[me], (ssem, rsem), k - 1, (z, lax.rem(me + k, PEERS))))
                 for k in range(1, PEERS)]
    for mv in vec_moves:
        mv.start()
    all_v[me] = vecs[:]
    get_wq.wait()
    stores, rounds = [], []

    def store(src, dst):
        cp = pltpu.make_async_copy(src, dst, lsem.at[len(loads) + len(stores)])
        cp.start()
        stores.append(cp)

    for t in range(3):
        part = slice(t * ROWS, (t + 1) * ROWS)
        own[part] = wq_s[:, t * D:(t + 1) * D].astype(BF16)
        mid = t * ROWS + ROWS // 2
        rounds.append(gather_moves(wall, (ssem, rsem), PEERS - 1 + t * GATHER_COPIES, own.at[part], part,
                                   (slice(t * ROWS, mid), slice(mid, (t + 1) * ROWS))))
        for mv in rounds[t][0].every:
            mv.start()
    store(own, wall.at[me])

    get_wo.wait()
    ff_own[DEPTH, :ROWS] = wo_s[:].astype(BF16)
    store(ff_own.at[DEPTH, pl.ds(0, ROWS)], wo_buf.at[me])
    get_up.wait()
    get_down.wait()
    for j, buf in enumerate(ff_bufs):
        for k in range(PEERS):
            ff_own[j, :ROWS, block(k)] = up_s[:, block(DEPTH * k + j)].astype(BF16)
        ff_own[j, ROWS:] = down_s[j * ROWS:(j + 1) * ROWS].astype(BF16)
        store(ff_own.at[j], buf.at[me])

    def by_sequence(t, out_ref):
        for k in range(PEERS):
            wide[k] = xs[t, :, :, block(k)].astype(F32).reshape(SEQ * NSEQ, LANES)
        out_ref[:, MAIN:PAD] = jnp.zeros((NSEQ, TAIL, D), BF16)

        @pl.loop(0, NSEQ)
        def _(s):
            for k in range(PEERS):
                out_ref[s, pl.ds(0, SEQ), block(k)] = wide[k, pl.ds(s, SEQ, stride=NSEQ), :].astype(BF16)

    get_x.wait()
    by_sequence(0, xp_ref)
    pass_on(rounds[:1], 1)
    get_g.wait()
    by_sequence(1, gp_ref)
    pass_on(rounds[1:], 1)
    for mv in vec_moves:
        mv.recv()
    for r in range(V_QKV):
        table_ref[r:r + 1] = jnp.concatenate([all_v[k, r:r + 1] for k in range(PEERS)], axis=1)
    flat = [all_v[k, V_QKV + t:V_QKV + t + 1] for k in range(PEERS) for t in range(3)]
    for t in range(3):
        table_ref[V_QKV + t:V_QKV + t + 1] = jnp.concatenate(flat[t * PEERS:(t + 1) * PEERS], axis=1)
    table_ref[:] = table_ref[:].astype(BF16).astype(F32)
    pass_on(rounds, 2)
    for first, second, third in rounds:
        for mv in first.kept + second.kept + third.every:
            mv.recv()
        for mv in first.every + second.every + third.every:
            mv.sent()
    for mv in vec_moves:
        mv.sent()
    for cp in stores:
        cp.wait()


def run_intake(xt, gt, wq, wo, wup, wdown, vecs, cid):
    copies = PEERS - 1 + 3 * GATHER_COPIES
    bufs = [jax.ShapeDtypeStruct((PEERS, n * ROWS, D), BF16) for n in (3, 1) + (2,) * DEPTH]
    vmem = pltpu.VMEM
    return pl.pallas_call(
        intake_kernel,
        in_specs=[ANY] * 6 + [pl.BlockSpec(memory_space=vmem)],
        out_specs=[pl.BlockSpec(memory_space=vmem)] * 2 + [ANY] * len(bufs) + [pl.BlockSpec(memory_space=vmem)],
        out_shape=[act(), act()] + bufs + [f32s(16, D)],
        scratch_shapes=[vmem((2, SEQ, NSEQ, D), BF16), vmem((PEERS, SEQ * NSEQ, LANES), F32),
                        vmem(wq.shape, F32), vmem(wo.shape, F32), vmem(wup.shape, F32), vmem(wdown.shape, F32),
                        vmem((3 * ROWS, D), BF16), vmem((DEPTH + 1, 2 * ROWS, D), BF16), vmem((PEERS, 16, LANES), F32),
                        pltpu.SemaphoreType.DMA((copies,)), pltpu.SemaphoreType.DMA((copies,)),
                        pltpu.SemaphoreType.DMA((6 + 2 + DEPTH,))],
        compiler_params=pltpu.CompilerParams(vmem_limit_bytes=VMEM_MAX, collective_id=cid, has_side_effects=True),
        name="intake",
    )(xt, gt, wq, wo, wup, wdown, vecs)


def qkv_kernel(traffic, x_ref, wq_ref, wk_ref, wv_ref, vec_ref, *refs):
    n_in, n_out, _ = traffic.sizes()
    srcs, (h_ref, q_ref, k_ref, v_ref, *refs) = refs[:n_in], refs[n_in:]
    i = pl.program_id(0)
    traffic.begin(i, srcs, refs[:n_out], refs[n_out:])
    rows = x_ref.shape[0] * PAD
    g1, c1, *_ = table_rows(vec_ref)
    xhat, _ = ln_fwd(x_ref[:].reshape(rows, D).astype(F32))
    h = (xhat * g1 + c1).astype(BF16)
    h_ref[:] = h.reshape(h_ref.shape)
    biases = table_rows(vec_ref, V_QKV, 3)
    for w_ref, o_ref, bias in zip((wq_ref, wk_ref, wv_ref), (q_ref, k_ref, v_ref), biases):
        o_ref[:] = (dot_nn(h, w_ref[:].reshape(D, D)) + bias).astype(BF16).reshape(o_ref.shape)
    traffic.finish(i == pl.num_programs(0) - 1)


def run_qkv(xp, wall, vec, cid, items):
    bs = 2
    traffic = Traffic(items)
    tok = pl.BlockSpec((bs, PAD, D), lambda s: (s, 0, 0))
    outs = pl.pallas_call(
        functools.partial(qkv_kernel, traffic), grid=(NSEQ // bs,),
        in_specs=[tok, *map(wblk, range(3)), fixed(vec.shape)] + traffic.in_specs(),
        out_specs=[tok] * 4 + traffic.out_specs(), out_shape=[act()] * 4 + traffic.out_shapes(),
        scratch_shapes=traffic.scratch(), input_output_aliases=traffic.aliases(5, 4),
        compiler_params=comm_params(cid), name="qkv",
    )(xp, wall, wall, wall, vec, *traffic.arrays())
    return outs[:4], traffic.split(outs[4:])


def low_lanes(rows):
    return lax.broadcasted_iota(jnp.int32, (rows, LANES), 1) < HEAD


def keys_mask(st):
    tail = st[MAIN:PAD]
    row = lax.broadcasted_iota(jnp.int32, tail.shape, 0)
    return jnp.concatenate([st[:MAIN], jnp.where(row < SEQ - MAIN, tail, NEG)], axis=0)


def diag_mask(heads):
    shape = (heads, heads * HEAD)
    row = lax.broadcasted_iota(jnp.int32, shape, 0)
    return lax.broadcasted_iota(jnp.int32, shape, 1) // HEAD == row


def last_by_head(t_ref, dmask, cols=slice(None)):
    last = t_ref[MAIN:PAD, cols][:1]
    return jnp.where(dmask, jnp.broadcast_to(last.astype(F32), dmask.shape), 0.0).astype(BF16)


def only_first_row(t):
    row = lax.broadcasted_iota(jnp.int32, (TAIL, t.shape[1]), 0)
    return jnp.where(row == 0, jnp.broadcast_to(t, row.shape), 0.0)


def softmax_t(st):
    st = keys_mask(st)
    m = jnp.max(st, axis=0, keepdims=True) * (SCALE * LOG2E)
    e = jnp.exp2(st * (SCALE * LOG2E) - m)
    total = col_sum(e)
    return e, total, m


def two_heads(t, low):
    zero = jnp.zeros(t.shape, t.dtype)
    return jnp.where(low, t, zero), jnp.where(low, zero, t)


def attn_fwd_kernel(traffic, q_ref, k_ref, v_ref, x_ref, g_ref, wo_ref, vec_ref, *refs):
    n_in, n_out, _ = traffic.sizes()
    srcs, (o_ref, a_ref, y_ref, h2_ref, dm_ref, lse_ref, *refs) = refs[:n_in], refs[n_in:]
    dsts, (s_s, p_s, *rest) = refs[:n_out], refs[n_out:]
    i = pl.program_id(0)
    traffic.begin(i, srcs, dsts, rest)
    low_q = low_lanes(MAIN)
    for p in range(HEADS // 2):
        halves = two_heads(q_ref[:MAIN, block(p)], low_q)
        for hh, qa in enumerate(halves):
            s_s[2 * p + hh] = dot_nt(k_ref[:, block(p)], qa)

    @pl.loop(0, ONCE)
    def _(t):
        for h in range(HEADS):
            e, total, m = softmax_t(s_s[h])
            p_s[h] = (e * (1.0 / total)).astype(BF16)
            lse_ref[h:h + 1, :] = m + jnp.log(total) * LOG2E

    for p in range(HEADS // 2):
        vt = v_ref[:, block(p)].T
        outs = [dot_nn(vt[hh * HEAD:(hh + 1) * HEAD], p_s[2 * p + hh]) for hh in range(2)]
        o_ref[:MAIN, block(p)] = jnp.concatenate(outs, axis=0).astype(BF16).T
    dmask = diag_mask(HEADS)
    e, total, _ = softmax_t(dot_nt(k_ref[:], last_by_head(q_ref, dmask)))
    ot = dot_tn((e * (1.0 / total)).astype(BF16), v_ref[:])
    o_ref[MAIN:PAD] = only_first_row(col_sum(jnp.where(dmask, ot, 0.0))).astype(BF16)

    _, _, bo, s1, g2, c2, _, s2 = table_rows(vec_ref)
    a = dot_nn(o_ref[:], wo_ref[:].reshape(D, D)) + bo
    a_ref[:] = a
    y = x_ref[:].astype(F32) + s1 * a
    y_ref[:] = y
    xhat, _ = ln_fwd(y)
    h2_ref[:] = (xhat * g2 + c2).astype(BF16)
    dm_ref[:] = (g_ref[:].astype(F32) * s2).astype(BF16)
    traffic.finish(i == NSEQ - 1)


def run_attn_fwd(q, k, v, xp, gp, wo, vec, cid, items):
    traffic = Traffic(items)
    tok = one_seq()
    outs = pl.pallas_call(
        functools.partial(attn_fwd_kernel, traffic), grid=(NSEQ,),
        in_specs=[tok] * 5 + [wblk(0), fixed(vec.shape)] + traffic.in_specs(),
        out_specs=[tok] * 5 + [pl.BlockSpec((None, HEADS, MAIN), lambda s: (s, 0, 0))] + traffic.out_specs(),
        out_shape=[act(), act(dtype=F32), act(dtype=F32), act(), act(), f32s(NSEQ, HEADS, MAIN)] + traffic.out_shapes(),
        scratch_shapes=[pltpu.VMEM((HEADS, PAD, MAIN), F32), pltpu.VMEM((HEADS, PAD, MAIN), BF16)] + traffic.scratch(),
        input_output_aliases=traffic.aliases(7, 6),
        compiler_params=comm_params(cid), name="attn_fwd",
    )(q, k, v, xp, gp, wo, vec, *traffic.arrays())
    return outs[:6], traffic.split(outs[6:])


def owner_rows(load, core):
    _, y, x, _ = coords()
    pieces = []
    for yy in (y, 1 - y):
        for xx in (x, 1 - x):
            pieces.append(load(pl.ds(pl.multiple_of((4 * yy + 2 * xx + core) * ROWS, ROWS), ROWS)))
    return jnp.concatenate(pieces, axis=1)


def store_piece(ab_ref, mine_ref, came_ref, unit):
    for color in range(2):
        for ry in range(2):
            for rx in range(2):
                r = 2 * ry + rx
                rows = slice(r * ROWS, (r + 1) * ROWS)
                sent, pos = (rx, ry) if color == 0 else (ry, rx)
                ab_ref[color, sent, pos, unit] = mine_ref[color, rows] + came_ref[color, rows]


class CorePair:
    def __init__(self, i, order, part_s, recv_s, sems):
        self.i, self.order, self.part_s, self.recv_s = i, order, part_s, recv_s
        self.slots = part_s.shape[0]
        self.sends = [[Move(remote(part_s.at[u % self.slots, n], recv_s.at[u, n], sems, 2 * u + n, partner("core")))
                       for n in range(2)] for u in range(recv_s.shape[0])]

    def before(self):
        for step, (what, u) in self.order.items():
            @pl.when(self.i == step)
            def _(step=step, what=what, u=u):
                came, prev = self.order.get(step - 1, ("none", 0))
                if came == "part":
                    self.sends[prev][1].start()
                if what == "mine":
                    for mv in self.sends[u]:
                        mv.sent()

    def product(self, u, left, right):
        theirs, mine = [next(st for st, which in self.order.items() if which == (what, u)) for what in ("part", "mine")]
        core = lax.rem(lax.axis_index("fsdp"), 2)

        @pl.when((self.i == theirs) | (self.i == mine))
        def _():
            who = jnp.where(self.i == mine, core, 1 - core)

            @pl.loop(0, 2)
            def _(n):
                @pl.when((self.i == theirs) & (n == 1))
                def _():
                    self.sends[u][0].start()
                cols = pl.ds(pl.multiple_of(n * HD, HD), HD)
                self.part_s[u % self.slots, n] = dot_tn(owner_rows(left, who), right(cols))

    def after(self, ab_ref, unit_of):
        for step, (what, u) in self.order.items():
            if what == "mine":
                @pl.when(self.i == step)
                def _(u=u):
                    for mv in self.sends[u]:
                        mv.recv()
                    store_piece(ab_ref, self.part_s.at[u % self.slots], self.recv_s.at[u], unit_of(u))


def pair_scratch(n):
    half = (2, 4 * ROWS, HD)
    return [pltpu.VMEM((2,) + half, F32), pltpu.VMEM((n,) + half, F32),
            pltpu.SemaphoreType.DMA((2 * n,)), pltpu.SemaphoreType.DMA((2 * n,))]


def piece_spec(width, n, before):
    return pl.BlockSpec((2, 2, 2, 1, ROWS, width // 2),
                        lambda i: (0, 0, 0, jnp.clip(i - before, 0, n - 1), 0, 0))


def mlp_kernel(first, row, traffic, h2_any, dm_any, wff_any, vec_ref, *refs):
    n_in, n_out, _ = traffic.sizes()
    if not first:
        m_in, dh_in, *refs = refs
    srcs, (m_out, dh_out, ab_ref, db_ref, *refs) = refs[:n_in], refs[n_in:]
    dsts, (h2_ref, dm_ref, w_s, load_sem, act_s, du_s, part_s, recv_s, core_send, core_recv, *rest) = refs[:n_out], refs[n_out:]
    i = pl.program_id(0)
    bs = m_out.shape[0]
    rows = bs * PAD
    nblk = NSEQ // bs
    traffic.begin(i, srcs, dsts, rest)

    loads = [pltpu.make_async_copy(wff_any.at[:, block(k)], w_s.at[k], load_sem.at[k]) for k in range(2)]
    w1_load, w2_load = loads

    def blocks(j):
        some = pl.ds(j * bs, bs)
        return [pltpu.make_async_copy(src.at[some], dst.at[some], load_sem.at[2 + 2 * j + k])
                for k, (src, dst) in enumerate(((h2_any, h2_ref), (dm_any, dm_ref)))]

    @pl.when(i == 0)
    def _():
        db_ref[:] = jnp.zeros_like(db_ref)
        h2_load, dm_load = blocks(0)
        for cp in (w1_load, h2_load, w2_load, dm_load):
            cp.start()
        for j in range(1, nblk):
            for cp in blocks(j):
                cp.start()

    for j in range(nblk):
        @pl.when(i == j)
        def _(j=j):
            for cp in blocks(j) + ([] if j else loads):
                cp.wait()

    @pl.when(i < nblk)
    def _():
        hb = h2_ref[pl.ds(i * bs, bs)].reshape(rows, D)
        dmb = dm_ref[pl.ds(i * bs, bs)].reshape(rows, D)
        w1 = w_s[0].reshape(D, QTR)
        w2 = w_s[1].reshape(QTR, D)
        mine = pl.ds(pl.multiple_of(i * rows, rows), rows)
        cw = 2 * LANES
        for c in range(QTR // cw):
            cols = slice(c * cw, (c + 1) * cw)
            u = dot_nn(hb, w1[:, cols]) + vec_ref[row:row + 1, cols]
            da = dot_nt(dmb, w2[cols])
            cdf = 0.5 + 0.5 * lax.erf(u * (0.5 ** 0.5))
            slope = cdf + u * (jnp.exp(-0.5 * u * u) * 0.3989422804014327)
            du = da * slope
            db_ref[:, cols] += sub8(du)
            act_s[mine, cols] = (u * cdf).astype(BF16)
            du_s[mine, cols] = du.astype(BF16)
        m = dot_nn(act_s[mine, :], w2).reshape(m_out.shape)
        dh = dot_nt(du_s[mine, :], w1).reshape(dh_out.shape)
        m_out[:] = m if first else m_in[:] + m
        dh_out[:] = dh if first else dh_in[:] + dh

    flat = NSEQ * PAD
    order = {nblk + 2 * k + u: (what, u) for k, what in enumerate(("part", "mine")) for u in range(2)}
    pair = CorePair(i, order, part_s, recv_s, (core_send, core_recv))
    pair.before()
    pair.product(0, lambda lanes: h2_ref[:, :, lanes].reshape(flat, ROWS), lambda cols: du_s[:, cols])
    pair.product(1, lambda lanes: act_s[:, lanes], lambda cols: dm_ref[:, :, cols].reshape(flat, cols.size))
    pair.after(ab_ref, lambda u: 0)
    traffic.finish(i == pl.num_programs(0) - 1)


def run_mlp(h2, dm, vec, wff, quarter, acc, cid, items):
    traffic = Traffic(items, ("core",))
    bs = 2
    nblk = NSEQ // bs
    tok = pl.BlockSpec((bs, PAD, D), lambda i: (jnp.minimum(i, nblk - 1), 0, 0))
    args = (h2, dm, wff, vec) + acc
    base = len(args)
    outs = pl.pallas_call(
        functools.partial(mlp_kernel, not acc, V_UP + quarter, traffic), grid=(nblk + 4,),
        in_specs=[ANY] * 3 + [fixed(vec.shape)] + [tok] * len(acc) + traffic.in_specs(),
        out_specs=[tok, tok, piece_spec(D, 2, nblk + 2), resident((8, QTR))] + traffic.out_specs(),
        out_shape=[act(dtype=F32), act(dtype=F32), f32s(2, 2, 2, 2, ROWS, HD), f32s(8, QTR)] + traffic.out_shapes(),
        scratch_shapes=[pltpu.VMEM(h2.shape, BF16), pltpu.VMEM(dm.shape, BF16), pltpu.VMEM((2, PEERS, ROWS, D), BF16),
                        pltpu.SemaphoreType.DMA((2 + 2 * nblk,))] + [pltpu.VMEM((NSEQ * PAD, QTR), BF16)] * 2
        + pair_scratch(2) + traffic.scratch(),
        input_output_aliases={**{base - len(acc) + k: k for k in range(len(acc))}, **traffic.aliases(base, 4)},
        compiler_params=comm_params(cid), name="mlp",
    )(*args, *traffic.arrays())
    m, dh, ab, db, *rest = outs
    return (m, dh), ab, db, traffic.split(rest)


ORDER = ("part0", "part1", "mine0", "part2", "mine1", "part3", "mine2", "mine3")
EARLY = 3
LOADED = ("o", "da", "h1", "dv", "dk", "dq")
LOADED_AT = ("o da", "h1 dv", "", "dk", "", "dq")


def wgrad_kernel(traffic, *refs):
    given, refs = refs[:len(LOADED)], refs[len(LOADED):]
    n_in, n_out, _ = traffic.sizes()
    srcs, (ab_ref, *refs) = refs[:n_in], refs[n_in:]
    early, refs = refs[:EARLY], refs[EARLY:]
    dsts, refs = refs[:n_out], refs[n_out:]
    here, refs = refs[:len(LOADED)], refs[len(LOADED):]
    load_sem, part_s, recv_s, core_send, core_recv, s1_send, s1_recv, *rest = refs
    i = pl.program_id(0)
    flat = NSEQ * PAD
    traffic.begin(i, srcs, dsts, rest)
    loads = [pltpu.make_async_copy(src, dst, load_sem.at[k]) for k, (src, dst) in enumerate(zip(given, here))]

    @pl.when(i == 0)
    def _():
        for cp in loads:
            cp.start()

    for step, some in enumerate(LOADED_AT):
        @pl.when(i == step)
        def _(some=some):
            for name in some.split():
                loads[LOADED.index(name)].wait()

    o, da, h1, dv, dk, dq = here
    units = ((o, da), (h1, dv), (h1, dk), (h1, dq))
    onward = [[Move(remote(ab_ref.at[color, 1, :, u], got.at[color], (s1_send, s1_recv), 2 * u + color, partner(nm)))
               for color, nm in enumerate(NAMES["s1"])] for u, got in enumerate(early)]
    order = {step: (name[:DEPTH], int(name[DEPTH:])) for step, name in enumerate(ORDER)}
    pair = CorePair(i, order, part_s, recv_s, (core_send, core_recv))
    pair.before()
    for step, (what, u) in order.items():
        if what == "mine" and u < EARLY:
            @pl.when(i == step + 1)
            def _(u=u):
                for mv in onward[u]:
                    mv.start()
    for u, (left, right) in enumerate(units):
        pair.product(u, lambda lanes, left=left: left[:, :, lanes].reshape(flat, ROWS),
                     lambda cols, right=right: right[:, :, cols].reshape(flat, cols.size))
    pair.after(ab_ref, lambda u: u)

    @pl.when(i == len(ORDER) - 1)
    def _():
        for moves in onward:
            for mv in moves:
                mv.recv()
                mv.sent()

    traffic.finish(i == len(ORDER) - 1)


def run_wgrad(ops, cid, items):
    traffic = Traffic(items, ("core", "x", "y"))
    n = DEPTH
    piece = (2, 2, 2, n, ROWS, HD)
    dma = pltpu.SemaphoreType.DMA
    outs = pl.pallas_call(
        functools.partial(wgrad_kernel, traffic), grid=(len(ORDER),),
        in_specs=[ANY] * len(ops) + traffic.in_specs(),
        out_specs=[fixed(piece)] + [ANY] * EARLY + traffic.out_specs(),
        out_shape=[f32s(*piece)] + [f32s(2, 2, ROWS, HD)] * EARLY + traffic.out_shapes(),
        scratch_shapes=[pltpu.VMEM(t.shape, BF16) for t in ops] + [dma((len(ops),))] + pair_scratch(n)
        + [dma((2 * EARLY,)), dma((2 * EARLY,))] + traffic.scratch(),
        input_output_aliases=traffic.aliases(len(ops), 1 + EARLY),
        compiler_params=comm_params(cid), name="wgrad",
    )(*ops, *traffic.arrays())
    ab, *outs = outs
    return ab, outs[:EARLY], traffic.split(outs[EARLY:])


def heads_bwd(half, q_ref, k_ref, v_ref, do_ref, lse_ref, dq_ref, dk_ref, dv_ref, sum_ref,
              dk_s, dv_s, s_s, dp_s, p_s, ds_s):
    low_q, low_k = low_lanes(MAIN), low_lanes(PAD)
    pairs = HH // 2
    cols = slice(half * HD, (half + 1) * HD)
    for p in range(pairs):
        lanes = block(half * pairs + p)
        queries = two_heads(q_ref[:MAIN, lanes], low_q)
        cots = two_heads(do_ref[:MAIN, lanes], low_q)
        for hh in range(2):
            s_s[2 * p + hh] = dot_nt(k_ref[:, lanes], queries[hh])
            dp_s[2 * p + hh] = dot_nt(v_ref[:, lanes], cots[hh])

    @pl.loop(0, ONCE)
    def _(t):
        for h in range(HH):
            dpt = dp_s[h]
            lse = lse_ref[half * HH + h:half * HH + h + 1, :]
            prob = jnp.exp2(keys_mask(s_s[h]) * (SCALE * LOG2E) - lse)
            p_s[h] = prob.astype(BF16)
            ds_s[h] = (prob * (dpt - col_sum(prob * dpt)) * SCALE).astype(BF16)

    dmask = diag_mask(HH)
    qb, dob = last_by_head(q_ref, dmask, cols), last_by_head(do_ref, dmask, cols)
    e, total, _ = softmax_t(dot_nt(k_ref[:, cols], qb))
    prob = e * (1.0 / total)
    dp = dot_nt(v_ref[:, cols], dob)
    ds = (prob * (dp - col_sum(prob * dp)) * SCALE).astype(BF16)
    dv_s[:] = dot_nn(prob.astype(BF16), dob)
    dk_s[:] = dot_nn(ds, qb)
    dq_tail = only_first_row(col_sum(jnp.where(dmask, dot_tn(ds, k_ref[:, cols]), 0.0)))
    dq_ref[MAIN:PAD, cols] = dq_tail.astype(BF16)
    sum_ref[0, :, cols] += sub8(dq_tail)

    for p in range(pairs):
        lanes = block(half * pairs + p)
        q2, do2 = q_ref[:MAIN, lanes], do_ref[:MAIN, lanes]
        kt = k_ref[:, lanes].T
        heads = range(2 * p, 2 * p + 2)
        dv = jnp.where(low_k, *[dot_nn(p_s[h], do2) for h in heads]) + dv_s[:, block(p)]
        dk = jnp.where(low_k, *[dot_nn(ds_s[h], q2) for h in heads]) + dk_s[:, block(p)]
        dq = jnp.concatenate([dot_nn(kt[hh * HEAD:(hh + 1) * HEAD], ds_s[h]) for hh, h in enumerate(heads)], axis=0).T
        dv_ref[:, lanes] = dv.astype(BF16)
        dk_ref[:, lanes] = dk.astype(BF16)
        dq_ref[:MAIN, lanes] = dq.astype(BF16)
        for k, t in enumerate((dq, dk, dv)):
            sum_ref[k, :, lanes] += sub8(t)


def heads_scratch():
    scores = (HH, PAD, MAIN)
    return [pltpu.VMEM((PAD, HD), F32), pltpu.VMEM((PAD, HD), F32), pltpu.VMEM(scores, F32), pltpu.VMEM(scores, F32),
            pltpu.VMEM(scores, BF16), pltpu.VMEM(scores, BF16)]


def back_kernel(traffic, m_ref, y_ref, dh_ref, a_ref, g_ref, q_ref, k_ref, v_ref, lse_ref, wo_ref, vec_ref, *refs):
    n_in, n_out, _ = traffic.sizes()
    srcs, (z_ref, gres_ref, da_ref, dq_ref, dk_ref, dv_ref, sum_ref, hsum_ref, *refs) = refs[:n_in], refs[n_in:]
    dsts, (do_s, *refs) = refs[:n_out], refs[n_out:]
    n = len(heads_scratch())
    heads = refs[:n]
    i = pl.program_id(0)
    traffic.begin(i, srcs, dsts, refs[n:])

    @pl.when(i == 0)
    def _():
        sum_ref[:] = jnp.zeros_like(sum_ref)
        hsum_ref[:] = jnp.zeros_like(hsum_ref)

    _, _, _, s1, g2, _, b2, s2 = table_rows(vec_ref)
    g = g_ref[:].astype(F32)
    y = y_ref[:]
    m = m_ref[:] + b2
    z_ref[:] = (y + s2 * m).astype(BF16)[:SEQ]
    dh = dh_ref[:]
    xhat, rstd = ln_fwd(y)
    gres = g + ln_bwd(dh * g2, xhat, rstd)
    gres_ref[:] = gres
    da = gres * s1
    for k, t in enumerate((da, gres * a_ref[:], dh * xhat, dh, g * s2, g * m)):
        sum_ref[k] += sub8(t)
    dab = da.astype(BF16)
    da_ref[:] = dab
    do_s[:] = dot_nt(dab, wo_ref[:].reshape(D, D)).astype(BF16)
    for half in range(2):
        heads_bwd(half, q_ref, k_ref, v_ref, do_s, lse_ref, dq_ref, dk_ref, dv_ref, hsum_ref, *heads)
    traffic.finish(i == NSEQ - 1)


def run_back(m, y, dh, a, gp, q, k, v, lse, wo, vec, cid, items):
    traffic = Traffic(items)
    tok = one_seq()
    outs = pl.pallas_call(
        functools.partial(back_kernel, traffic), grid=(NSEQ,),
        in_specs=[tok] * 8 + [pl.BlockSpec((None, HEADS, MAIN), lambda s: (s, 0, 0)), wblk(0), fixed(vec.shape)]
        + traffic.in_specs(),
        out_specs=[pl.BlockSpec((None, SEQ, D), lambda s: (s, 0, 0))] + [tok] * 5
        + [resident((6, 8, D)), resident((3, 8, D))] + traffic.out_specs(),
        out_shape=[jax.ShapeDtypeStruct((NSEQ, SEQ, D), BF16), act(dtype=F32)] + [act()] * 4
        + [f32s(6, 8, D), f32s(3, 8, D)] + traffic.out_shapes(),
        scratch_shapes=[pltpu.VMEM((PAD, D), BF16)] + heads_scratch() + traffic.scratch(),
        input_output_aliases=traffic.aliases(11, 8),
        compiler_params=comm_params(cid), name="back",
    )(m, y, dh, a, gp, q, k, v, lse, wo, vec, *traffic.arrays())
    return outs[:8], traffic.split(outs[8:])


def adds_kernel(n, *refs):
    ins, outs = refs[:2 * n], refs[2 * n:]
    for a_ref, b_ref, o_ref in zip(ins[::2], ins[1::2], outs):
        o_ref[:] = a_ref[:].reshape(o_ref.shape) + b_ref[:].reshape(o_ref.shape)


def quarters(shape, kept=False):
    *lead, rows, width = shape
    lead = (1,) + ((1,) + tuple(lead[2:]) if kept else tuple(lead[1:]))
    zeros = (0,) * (len(lead) - 1)
    return pl.BlockSpec(lead + (rows // 2, width), lambda g: (g // 2,) + zeros + (lax.rem(g, 2), 0))


def run_adds(*jobs):
    specs, outs = [], []
    for a, b in jobs:
        outs.append(quarters(b.shape))
        specs += [quarters(a.shape, a.ndim > b.ndim), outs[-1]]
    return pl.pallas_call(
        functools.partial(adds_kernel, len(jobs)), grid=(4,), in_specs=specs, out_specs=outs,
        out_shape=[f32s(*b.shape) for _, b in jobs],
        compiler_params=params(), name="adds",
    )(*[t for job in jobs for t in job])


def store_ff(gup_ref, gdown_ref, f_ref, j):
    half = PEERS // 2
    for k in range(PEERS):
        gup_ref[:, block(DEPTH * k + j)] = f_ref[k // half, 0, :, block(k % half)]
    for color in range(2):
        gdown_ref[j * ROWS:(j + 1) * ROWS, color * HD:(color + 1) * HD] = f_ref[color, 1]


UNITS = DEPTH
EVENTS = ("", "", "b0", "b1", "p00", "b2 p01", "p10 q00", "a3 p11 q01")


def finish_kernel(x_ref, gres_ref, dq_ref, dk_ref, dv_ref, wall_any, f0, f1, f2, vec_ref, ab_any, keep_ref, e0, e1, e2,
                  p3_ref, b3_ref, sum_ref, hsum_ref, db0, db1, db2, db3,
                  dx_ref, gqkv_ref, gout_ref, gup_ref, gdown_ref, small_ref,
                  w_s, f_s, load_sem, dx_s, ln_s, sk, r2, ra, rb, f3_s, small_s, all_p, part_s, all_z, ssem, rsem):
    i = pl.program_id(0)
    z, me = lax.axis_index("rep"), lax.axis_index("fsdp")
    sems, used = (ssem, rsem), []
    colors = range(2)

    def move(src, dst, device, *roles):
        used.append(Move(remote(src, dst, sems, len(used), device), *roles))
        return used[-1]

    s1 = {u: [move(ab_any.at[color, 1, :, u], sk.at[u, color], partner(nm)) for color, nm in enumerate(NAMES["s1"])]
          for u in range(EARLY, UNITS)}
    s2 = [[move(sk.at[u, color, 1], r2.at[u, color], partner(nm)) for color, nm in enumerate(NAMES["s2"])]
          for u in range(UNITS)]
    w_loads = [pltpu.make_async_copy(wall_any.at[:, block(k)], w_s.at[k], load_sem.at[k]) for k in range(3)]
    f_loads = [pltpu.make_async_copy(f, f_s.at[k], load_sem.at[3 + k]) for k, f in enumerate((f0, f1, f2))]
    near, far = partner("near"), partner("far")
    z_a = [[move(sk.at[u, c, 0], ra.at[u, c], near, *ROLES["zA"]) for c in colors] for u in range(UNITS)]
    z_b = [[move(ra.at[u, c], rb.at[u, c], far, *ROLES["zB"]) for c in colors] for u in range(UNITS)]
    z_c = [[move(rb.at[u, c], rb.at[u, c], near, *ROLES["zC"]) for c in colors] for u in range(UNITS)]
    f3_c = move(f3_s, f3_s, near, *ROLES["zC"])
    others = [(z, lax.rem(me + k, PEERS)) for k in range(1, PEERS)]
    column = [(lax.rem(z + k, DEPTH), me) for k in range(1, DEPTH)]
    plane_moves = [move(small_s.at[to], all_p.at[me], (zz, to)) for zz, to in others]
    column_moves = [move(part_s, all_z.at[z], dev) for dev in column]

    def start(moves):
        for mv in moves:
            mv.start()

    def arrive(moves):
        for mv in moves:
            mv.recv()

    def inner(do):
        pl.when(is_inner() == 1)(do)

    def after_s1(u, came=None):
        if came is None:
            arrive(s1[u])
        for pos in (1, 0):
            for c in colors:
                got = sk[u, c, pos] if came is None else came[c, pos]
                sk[u, c, pos] = got + keep_ref[c, 0, pos, u]
        start(s2[u])

    def after_s2(u):
        arrive(s2[u])
        for c in colors:
            sk[u, c, 0] = sk[u, c, 0] + r2[u, c]
        start(z_a[u])

    def after_za(u, c):
        arrive([z_a[u][c]])

        @inner
        def _():
            ra[u, c] = ra[u, c] + sk[u, c, 0]
        start([z_b[u][c]])

    def after_zb(u, c):
        arrive([z_b[u][c]])

        @inner
        def _():
            rb[u, c] = rb[u, c] + ra[u, c]
        start([z_c[u][c]])

    @pl.when(i == 0)
    def _():
        greet(others + column)
        ln_s[:] = jnp.zeros_like(ln_s)

        @inner
        def _():
            f3_s[:] = p3_ref[:] + b3_ref[:]
        start([f3_c])
        for u, came in enumerate((e0, e1, e2)):
            after_s1(u, came)
        for u in s1:
            start(s1[u])
        for cp in w_loads + f_loads:
            cp.start()
        for cp in w_loads:
            cp.wait()

    act_on = {"a": after_s1, "b": after_s2, "p": after_za, "q": after_zb}

    def handle(events):
        for kind, *which in events.split():
            act_on[kind](*map(int, which))

    for step, events in enumerate(EVENTS):
        @pl.when(i == step)
        def _(events=events):
            handle(events)

    dh = None
    for k, d_ref in enumerate((dq_ref, dk_ref, dv_ref)):
        part = dot_nt(d_ref[:], w_s[k].reshape(D, D))
        dh = part if dh is None else dh + part
    g1, *_ = table_rows(vec_ref)
    xhat, rstd = ln_fwd(x_ref[:].astype(F32))
    for k, t in enumerate((dh * xhat, dh)):
        ln_s[k] += sub8(t)
    dx = gres_ref[:] + ln_bwd(dh * g1, xhat, rstd)
    for k in range(PEERS):
        dx_s[k, pl.ds(i, SEQ, stride=NSEQ), :] = dx[:SEQ, block(k)]

    @pl.when(i == NSEQ - 1)
    def _():
        rows = [col_sum(ref[k]) for ref in (ln_s, sum_ref) for k in range(ref.shape[0])]
        rows += [col_sum(ref[:]) for ref in (db0, db1, db2, db3)]
        blocks = [col_sum(hsum_ref[t])[:, block(k)] for t in range(3) for k in range(PEERS)]
        for to in range(PEERS):
            mine = [row[:, block(to)] for row in rows] + blocks[3 * to:3 * to + 3] + [jnp.zeros((1, LANES), F32)]
            small_s[to] = jnp.concatenate(mine, axis=0)
        start(plane_moves)
        all_p[me] = small_s[me]
        for k in range(PEERS):
            dx_ref[:, :, block(k)] = dx_s[k].reshape(SEQ, NSEQ, LANES).astype(BF16)
        handle("q10 b3")
        arrive(plane_moves)
        part_s[:] = jnp.sum(all_p[:], axis=0)
        all_z[z] = part_s[:]
        start(column_moves)
        handle("p20 q11")
        for j, cp in enumerate(f_loads):
            cp.wait()
            store_ff(gup_ref, gdown_ref, f_s.at[j], j)
        handle("p21 q20")
        arrive([f3_c])
        store_ff(gup_ref, gdown_ref, f3_s, 3)
        arrive(column_moves)
        small_ref[:] = jnp.sum(all_z[:], axis=0)
        handle("p30 q21")
        handle("p31 q30 q31")
        for u, (out_ref, base) in enumerate(((gout_ref, 0), (gqkv_ref, 2 * D), (gqkv_ref, D), (gqkv_ref, 0))):
            for c in colors:
                arrive(z_c[u][c:c + 1])
                out_ref[:, base + c * HD:base + (c + 1) * HD] = rb[u, c]
        for mv in used:
            mv.sent()


def run_finish(xp, gres, grads, wall, vec, ab, early, ffs, last, sums, hsum, dbs, cid):
    tok = one_seq()
    outs = [(SEQ, NSEQ, D), (ROWS, 3 * D), (ROWS, D), (ROWS, DEPTH * D), (DEPTH * ROWS, D), (16, LANES)]

    def piece(*lead):
        return pltpu.VMEM(lead + (ROWS, HD), F32)

    scratch = [pltpu.VMEM((3, PEERS, ROWS, D), BF16), piece(3, 2, 2), pltpu.SemaphoreType.DMA((6,))]
    scratch += [pltpu.VMEM((PEERS, SEQ * NSEQ, LANES), F32), pltpu.VMEM((2, 8, D), F32)]
    scratch += [piece(UNITS, 2, 2)] + [piece(UNITS, 2)] * 3 + [piece(2, 2)]
    scratch += [pltpu.VMEM((PEERS, 16, LANES), F32)] * 2
    scratch += [pltpu.VMEM((16, LANES), F32), pltpu.VMEM((DEPTH, 16, LANES), F32)]
    scratch += [pltpu.SemaphoreType.DMA((64,)), pltpu.SemaphoreType.DMA((64,))]
    consts = [sums, hsum] + list(dbs)
    held = [*early, *last]
    before = [xp, gres, *grads, wall, *ffs, vec, ab, ab, *held]
    return pl.pallas_call(
        finish_kernel, grid=(NSEQ,),
        in_specs=[tok] * 5 + [ANY] * 4 + [fixed(vec.shape), ANY, kept_spec(ab.shape)]
        + [fixed(t.shape) for t in held + consts],
        out_specs=[fixed(sh) for sh in outs],
        out_shape=[jax.ShapeDtypeStruct(outs[0], BF16)] + [f32s(*sh) for sh in outs[1:]],
        scratch_shapes=scratch, compiler_params=comm_params(cid), name="finish",
    )(*before, *consts)


def device_step(x_loc, dz_loc, w_qkv, b_qkv, w_out, w_up, b_up, w_down, vec_params):
    cid = itertools.count()
    vecs = jnp.concatenate([vec_params, b_up.reshape(-1, LANES), b_qkv.reshape(-1, LANES), jnp.zeros((1, LANES), F32)])
    xp, gp, wall, wo, c0, c1, c2, c3, vec = run_intake(
        x_loc.swapaxes(0, 1), dz_loc.swapaxes(0, 1), w_qkv, w_out, w_up, w_down, vecs, next(cid))
    own, rest = range(2)
    (h1, q, k, v), (wo,) = run_qkv(xp, wall, vec, next(cid), [Gather(wo, own, 2, 3)])
    (o, a, y, h2, dm, lse), (c0, c1) = run_attn_fwd(
        q, k, v, xp, gp, wo, vec, next(cid), [Gather(c0, own, 3, 5), Gather(c1, own, start=3)])

    mlp = functools.partial(run_mlp, h2, dm, vec)
    acc, f0, db0, (c1, c2, c3) = mlp(c0, 0, (), next(cid), [Gather(c1, rest, 3), Gather(c2, own), Gather(c3, own)])
    acc, f1, db1, (c2, c3, r0) = mlp(
        c1, 1, acc, next(cid), [Gather(c2, rest, 3), Gather(c3, rest, 4), Chain(f0, "s1")])
    f0, = run_adds((f0, r0))
    acc, f2, db2, (r0, r1) = mlp(c2, 2, acc, next(cid), [Chain(f0, "s2", ("zA", 2)), Chain(f1, "s1")])
    f1, f0 = run_adds((f1, r1), r0)
    acc, f3, db3, (r1, r2, r0) = mlp(
        c3, 3, acc, next(cid), [Chain(f1, "s2", ("zA", 2)), Chain(f2, "s1"), Chain(f0, "zB")])
    f2, f1, f0 = run_adds((f2, r2), r1, (f0, r0))
    m, dh = acc
    (z, gres, da, dq, dk, dv, sums, hsum), (r2, r3, f1, f0) = run_back(
        m, y, dh, a, gp, q, k, v, lse, wo, vec, next(cid),
        [Chain(f2, "s2", ("zA", 2), ("zB", 4, 6)), Chain(f3, "s1", ("s2", 6)), Chain(f1, "zB", ("zC", 2, 4)), Chain(f0, "zC")])
    f3, f2 = run_adds(r3, r2)
    ab, early, (r3, f2) = run_wgrad([o, da, h1, dv, dk, dq], next(cid), [Chain(f3, "zA", ("zB", 5, 7)), Chain(f2, "zC")])
    dx, g_qkv, g_out, g_up, g_down, small = run_finish(
        xp, gres, [dq, dk, dv], wall, vec, ab, early, [f0, f1, f2], r3, sums, hsum, [db0, db1, db2, db3], next(cid))
    g_bup, g_bqkv = small[V_UP:V_QKV].reshape(-1), small[V_QKV:V_QKV + 3].reshape(-1)
    return z, dx.swapaxes(0, 1), g_qkv, g_bqkv, g_out, g_up, g_bup, g_down, small[:V_UP]


def solution(mesh):
    batch = P(("rep", "fsdp"), None, None)
    row, flat, col = P("fsdp", None), P("fsdp"), P(None, "fsdp")
    par = (row, flat, row, row, flat, row, col)
    return jax.shard_map(device_step, mesh=mesh, in_specs=(batch, batch) + par,
                         out_specs=(batch, batch) + par, check_vma=False)
```
